256 devices in a mesh: replica: 16 (over y_hi, x, core), model: 16 (over z, y_lo).
Axes of the slice: x: 4, y: 4 (y_hi: 2, y_lo: 2; y = y_hi * 2 + y_lo), z: 8, core: 2. Of those that a mesh axis runs over, the one named last changes fastest.
Arguments:
- slope_gate: float32 [16, 2048, 6144], P('replica', None, 'model'), may hold values from -0.875 to 0.875
- slope_up: float32 [16, 2048, 6144], P('replica', None, 'model'), may hold values from -0.875 to 0.875
- slope_down: float32 [16, 6144, 2048], P('replica', 'model'), may hold values from -0.875 to 0.875
- slope_norm: float32 [16, 2048], P('replica'), may hold values from -8 to 8
- param_gate: float32 [2048, 6144], P('replica', 'model'), may hold values from -0.1875 to 0.1875
- param_up: float32 [2048, 6144], P('replica', 'model'), may hold values from -0.1875 to 0.1875
- param_down: float32 [6144, 2048], P('model', 'replica'), may hold values from -0.109375 to 0.109375
- param_norm: float32 [2048], P('replica'), may hold values from 0.25 to 1.75
Outputs:
- half_gate: bfloat16 [2048, 6144], P(None, 'model')
- half_up: bfloat16 [2048, 6144], P(None, 'model')
- half_down: bfloat16 [6144, 2048], P('model')
- half_norm: bfloat16 [2048], replicated
- next_gate: float32 [2048, 6144], P('replica', 'model')
- next_up: float32 [2048, 6144], P('replica', 'model')
- next_down: float32 [6144, 2048], P('model', 'replica')
- next_norm: float32 [2048], P('replica')
The draws below stay inside these ranges and needn't reach their ends.
All inputs are finite; a program needn't handle non-finite values.
Results may differ from the reference program's by a relative error of at most 0.0004.
Values may be sent and summed in bfloat16 or wider, within the bound.
A program may use at most 128 MiB of HBM per device.

```python
import jax
import jax.numpy as jnp
from jax import lax

WIDTH = 2048
INNER = 6144
REPLICAS = 16


def strengthened(values, stream_key, source, target, shards_of, factor):
    owner, partner = [(jnp.arange(values.shape[dim]) // (values.shape[dim] // shards_of)).reshape([-1 if axis == dim else 1 for axis in range(values.ndim)]) for dim in (source, target)]
    chosen = jax.random.permutation(stream_key, shards_of)[partner]
    strong = (owner == chosen) | (owner == (partner + shards_of // 2) % shards_of)
    return jnp.where(strong, factor * values, values)


def levels(stream_key, shape, cuts, low, top_value):
    def one(dim, parts):
        draws = jax.random.uniform(jax.random.fold_in(jax.random.fold_in(stream_key, 6), dim), (parts,), jnp.float32, low / len(cuts), top_value / len(cuts))
        return jnp.repeat(jnp.exp(draws), shape[dim] // parts).reshape((-1,) + (1,) * (len(shape) - dim - 1))

    factor_of = one(*cuts[0])
    for cut in cuts[1:]:
        factor_of = factor_of * one(*cut)
    return factor_of


def noise_with(key, dims, width, most, shards, heavy, dtype=jnp.bfloat16):
    drawn = width * jax.random.normal(key, dims, jnp.float32)
    if shards:
        drawn = drawn * levels(key, dims, shards, -0.22, 0.18)
    return jnp.clip(strengthened(drawn, jax.random.fold_in(key, 3), *heavy), -most, most).astype(dtype)


def setup_inputs(seed: int = 0) -> dict:
    arg_keys = jax.random.split(jax.random.key(seed), 9)
    return {
        "slope_gate": noise_with(arg_keys[0], (REPLICAS, WIDTH, INNER), 0.1, 0.875, ((0, 16), (2, 16)), (0, 1, 16, 2.0), jnp.float32),
        "slope_up": noise_with(arg_keys[1], (REPLICAS, WIDTH, INNER), 0.1, 0.875, ((0, 16), (2, 16)), (0, 1, 16, 2.0), jnp.float32),
        "slope_down": noise_with(arg_keys[2], (REPLICAS, INNER, WIDTH), 0.1, 0.875, ((0, 16), (1, 16)), (0, 2, 16, 2.0), jnp.float32),
        "slope_norm": noise_with(arg_keys[3], (REPLICAS, WIDTH), 1.0, 8.0, ((0, 16),), (0, 1, 16, 2.0), jnp.float32),
        "param_gate": noise_with(arg_keys[4], (WIDTH, INNER), WIDTH ** -0.5, 0.1875, ((0, 16), (1, 16)), (1, 0, 16, 2.0), jnp.float32),
        "param_up": noise_with(arg_keys[5], (WIDTH, INNER), WIDTH ** -0.5, 0.1875, ((0, 16), (1, 16)), (1, 0, 16, 2.0), jnp.float32),
        "param_down": noise_with(arg_keys[6], (INNER, WIDTH), INNER ** -0.5, 0.109375, ((0, 16), (1, 16)), (0, 1, 16, 2.0), jnp.float32),
        "param_norm": jnp.clip(1.0 + 0.15 * jax.random.normal(arg_keys[7], (WIDTH,), jnp.float32), 0.25, 1.75),
    }


learn_rate = 0.5

def reference(slope_gate, slope_up, slope_down, slope_norm, param_gate, param_up, param_down, param_norm):
    mean_gate = lax.optimization_barrier(jnp.sum(slope_gate.astype(jnp.float32), axis=0)) * REPLICAS ** (-0.5)
    mean_up = lax.optimization_barrier(jnp.sum(slope_up.astype(jnp.float32), axis=0)) * REPLICAS ** (-0.5)
    mean_down = lax.optimization_barrier(jnp.sum(slope_down.astype(jnp.float32), axis=0)) * REPLICAS ** (-0.5)
    mean_norm = lax.optimization_barrier(jnp.sum(slope_norm.astype(jnp.float32), axis=0)) * REPLICAS ** (-0.5)
    ratio_gate = jnp.sqrt(lax.optimization_barrier(jnp.sum(param_gate * param_gate, axis=1, keepdims=True))) * lax.rsqrt(lax.optimization_barrier(jnp.sum(mean_gate * mean_gate, axis=1, keepdims=True)) + 1e-06)
    mean_gate = mean_gate * ratio_gate
    ratio_up = jnp.sqrt(lax.optimization_barrier(jnp.sum(param_up * param_up, axis=1, keepdims=True))) * lax.rsqrt(lax.optimization_barrier(jnp.sum(mean_up * mean_up, axis=1, keepdims=True)) + 1e-06)
    mean_up = mean_up * ratio_up
    ratio_down = jnp.sqrt(lax.optimization_barrier(jnp.sum(param_down * param_down, axis=0, keepdims=True))) * lax.rsqrt(lax.optimization_barrier(jnp.sum(mean_down * mean_down, axis=0, keepdims=True)) + 1e-06)
    mean_down = mean_down * ratio_down
    next_gate = param_gate - learn_rate * mean_gate
    next_up = param_up - learn_rate * mean_up
    next_down = param_down - learn_rate * mean_down
    next_norm = param_norm - learn_rate * mean_norm
    half_gate = next_gate.astype(jnp.bfloat16)
    half_up = next_up.astype(jnp.bfloat16)
    half_down = next_down.astype(jnp.bfloat16)
    half_norm = next_norm.astype(jnp.bfloat16)
    return (half_gate, half_up, half_down, half_norm, next_gate, next_up, next_down, next_norm)
```

```python
import functools

import jax
import jax.numpy as jnp
from jax import lax
from jax.experimental import pallas as pl
from jax.experimental.pallas import tpu as pltpu
from jax.sharding import PartitionSpec as P

MESH = pl.DeviceIdType.MESH
LEARN_RATE = 0.5
EPS = 1e-06
ROWS = 128
XS = 4


class Copies:
    def __init__(self, send, recv):
        self.send, self.recv, self.used, self.started = send, recv, 0, []

    def start(self, src, dst, target):
        copy = pltpu.make_async_remote_copy(
            src_ref=src,
            dst_ref=dst,
            send_sem=self.send.at[self.used],
            recv_sem=self.recv.at[self.used],
            device_id=target,
            device_id_type=MESH,
        )
        copy.start()
        self.used += 1
        self.started.append(copy)
        return copy

    def drain(self):
        for copy in self.started:
            copy.wait_send()


class Tensor:
    def __init__(self, by_rows, x_first, slope, param, half, new, scratch):
        self.by_rows, self.x_first = by_rows, x_first
        self.slope, self.param, self.half, self.new = slope, param, half, new
        (self.s, self.r, self.f, self.d, self.a, self.y, self.p, self.src, self.nm) = scratch
        self.block = self.p.shape

    def share(self, ref, index):
        at = pl.ds(pl.multiple_of(index * ROWS, ROWS), ROWS)
        return ref.at[at, :] if self.by_rows else ref.at[:, at]

    def part(self, ref, index, h):
        size = self.block[0] // 2
        if self.by_rows:
            return ref.at[pl.ds(pl.multiple_of(index * ROWS + h * size, size), size), :]
        return ref.at[pl.ds(h * size, size), pl.ds(pl.multiple_of(index * ROWS, ROWS), ROWS)]

    def item(self, yh, h, x):
        if self.x_first:
            return self.s.at[h, x]
        size = self.block[0] // 2
        return self.s.at[yh, x, pl.ds(h * size, size), :]

    def squares(self, value):
        value = value * value
        if not self.by_rows:
            return jnp.sum(value, axis=0, keepdims=True)
        folded = value[:, :ROWS]
        for at in range(ROWS, value.shape[1], ROWS):
            folded = folded + value[:, at : at + ROWS]
        return jnp.sum(folded.T, axis=0, keepdims=True)


def add(into, *others):
    value = into[...]
    for other in others:
        value = value + other[...]
    into[...] = value


def kernel(replicas, models, *refs):
    (sg, su, sd, sn, pg, pu, pd, pn), refs = refs[:8], refs[8:]
    (hg, hu, hd, hn, ng, nu, nd, nn), refs = refs[:8], refs[8:]
    ta, refs = Tensor(True, True, sg, pg, hg, ng, refs[:9]), refs[9:]
    ty, refs = Tensor(True, False, su, pu, hu, nu, refs[:9]), refs[9:]
    tb, refs = Tensor(False, True, sd, pd, hd, nd, refs[:9]), refs[9:]
    nv_src, nv_dst, nn_src, nn_dst, local_sem, send_sem, recv_sem = refs

    r = lax.axis_index("replica")
    m = lax.axis_index("model")
    core = r % 2
    x = (r // 2) % XS
    yh = r // (2 * XS)
    yo = 1 - yh
    xr, xl, x2 = (x + 1) % XS, (x + XS - 1) % XS, (x + 2) % XS

    def owner(y, xx, c):
        return (y * XS + xx) * 2 + c

    def device(y, xx, c):
        return {"replica": owner(y, xx, c), "model": m}

    right, left = device(yh, xr, core), device(yh, xl, core)
    across, partner = device(yo, x, core), device(yh, x, 1 - core)
    net = Copies(send_sem, recv_sem)

    order = [(ta, 0, x2), (ta, 1, x2), (ty, yo, x2), (ta, 1, xr), (ta, 0, xl), (ty, yo, xr)]
    order += [(ta, 0, xr), (ta, 1, xl), (ty, yo, xl), (tb, 0, x2), (tb, 1, x2)]
    order += [(ty, yh, x2), (ty, yh, xr), (ta, yo, x), (ta, yh, x), (tb, 1, xr), (tb, 0, xl)]
    order += [(ty, yh, xl), (ty, yo, x), (tb, 0, xr), (tb, 1, xl), (ty, yh, x)]
    order += [(tb, yo, x), (tb, yh, x)]
    loads = []
    for i, (t, y, xx) in enumerate(order):
        copy = pltpu.make_async_copy(
            t.share(t.slope.at[0], owner(y, xx, core)), t.s.at[y, xx], local_sem.at[i]
        )
        copy.start()
        loads.append(copy)
    params = []
    for i, t in enumerate((ta, ty, tb)):
        copy = pltpu.make_async_copy(t.param, t.p, local_sem.at[len(order) + i])
        copy.start()
        params.append(copy)
    for i in range(replicas):
        nv_src[i, 0:1, :] = sn[0:1, i * ROWS : (i + 1) * ROWS]

    barrier = pltpu.get_barrier_semaphore()
    peers = [{"replica": (r + k) % replicas, "model": m} for k in range(1, replicas)]
    others = [{"replica": r, "model": (m + k) % models} for k in range(1, models)]
    for peer in peers + others:
        pl.semaphore_signal(barrier, inc=1, device_id=peer, device_id_type=MESH)
    pl.semaphore_wait(barrier, replicas + models - 2)

    swaps = []
    for t, y, xx in order:
        swaps.append(
            net.start(t.share(t.slope.at[0], owner(y, xx, 1 - core)), t.r.at[y, xx], partner)
        )
    vectors = []
    for k, peer in enumerate(peers, 1):
        vectors.append(
            net.start(nv_src.at[peer["replica"], pl.ds(0, 1)], nv_dst.at[k, pl.ds(0, 1)], peer)
        )

    taken = [0]

    def take(count):
        for i in range(taken[0], taken[0] + count):
            t, y, xx = order[i]
            loads[i].wait()
            swaps[i].wait_recv()
            add(t.s.at[y, xx], t.r.at[y, xx])
        taken[0] += count

    def far(t):
        return (
            net.start(t.item(yh, 0, x2), t.f.at[0], right),
            net.start(t.item(yh, 1, x2), t.f.at[1], left),
        )

    def near(t):
        return (
            net.start(t.item(yh, 0, xl), t.d.at[0], left),
            net.start(t.item(yh, 1, xr), t.d.at[1], right),
        )

    def relay(t, got):
        got[0].wait_recv()
        add(t.item(yh, 0, xr), t.f.at[0])
        first = net.start(t.item(yh, 0, xr), t.a.at[0], right)
        got[1].wait_recv()
        add(t.item(yh, 1, xl), t.f.at[1])
        return first, net.start(t.item(yh, 1, xl), t.a.at[1], left)

    def settle(t, direct, relayed):
        for h in (0, 1):
            direct[h].wait_recv()
        for h in (0, 1):
            relayed[h].wait_recv()
            add(t.item(yh, h, x), t.d.at[h], t.a.at[h])

    def finish(t, extra=()):
        own = t.s.at[yh, x]
        value = own[...]
        for e in extra:
            value = value + e[...]
        value = value * (replicas**-0.5)
        own[...] = value
        t.src[0:1, :] = t.squares(value)
        sent = [
            net.start(t.src, t.nm.at[k], peer) for k, peer in enumerate(others, 1)
        ]
        return sent

    def update(t, sent):
        total = t.src[...]
        for copy in sent:
            copy.wait_recv()
        for k in range(1, models):
            total = total + t.nm[k]
        ratio = jnp.sqrt(total[1:2]) * lax.rsqrt(total[0:1] + EPS)
        if t.by_rows:
            ratio = jnp.broadcast_to(ratio, (ROWS, ROWS)).T
            ratio = jnp.concatenate([ratio] * (t.block[1] // ROWS), axis=1)
        new = t.p[...] - LEARN_RATE * (t.s[yh, x] * ratio)
        t.new[...] = new
        t.share(t.half, owner(yh, x, core))[...] = new.astype(jnp.bfloat16)

    def blk(t, y, xx):
        return t.share(t.half, owner(y, xx, core))

    def spread(t, y, xx, target):
        return net.start(blk(t, y, xx), blk(t, y, xx), target)

    handed = []

    def hand(t, y, xx):
        handed.append(spread(t, y, xx, partner))

    take(2)
    a_far = far(ta)
    take(1)
    y_got = [net.start(ty.s.at[yo, x2], ty.y.at[0], across)]
    take(2)
    a_near = near(ta)
    take(1)
    y_got.append(net.start(ty.s.at[yo, xr], ty.y.at[1], across))
    take(3)
    y_got.append(net.start(ty.s.at[yo, xl], ty.y.at[2], across))
    take(2)
    for t, copy in zip((ta, ty, tb), params):
        copy.wait()
        t.src[1:2, :] = t.squares(t.p[...])
    take(2)
    a_relay = relay(ta, a_far)
    b_far = far(tb)
    take(4)
    b_near = near(tb)
    take(7)

    mean = nv_src[r, 0:1, :]
    for k, copy in enumerate(vectors, 1):
        copy.wait_recv()
        mean = mean + nv_dst[k, 0:1, :]
    new = pn[...] - LEARN_RATE * (mean * (replicas**-0.5))
    nn[...] = new
    nn_src[0:1, :] = new
    nn_dst[r, 0:1, :] = new
    gathered = [
        net.start(nn_src.at[pl.ds(0, 1)], nn_dst.at[r, pl.ds(0, 1)], peer) for peer in peers
    ]

    y_got[0].wait_recv()
    add(ty.s.at[yh, x2], ty.y.at[0])
    y_got[1].wait_recv()
    add(ty.s.at[yh, xr], ty.y.at[1])
    settle(ta, a_near, a_relay)
    a_y = net.start(ta.s.at[yo, x], ta.y, across)
    y_got.append(net.start(ty.s.at[yo, x], ty.y.at[3], across))
    y_got[2].wait_recv()
    add(ty.s.at[yh, xl], ty.y.at[2])
    b_relay = relay(tb, b_far)
    y_far = far(ty)
    y_near = near(ty)
    a_y.wait_recv()
    a_norm = finish(ta, (ta.y,))
    y_got[3].wait_recv()
    add(ty.s.at[yh, x], ty.y.at[3])
    update(ta, a_norm)
    a_up = spread(ta, yh, x, across)
    hand(ta, yh, x)
    settle(tb, b_near, b_relay)
    b_y = net.start(tb.s.at[yo, x], tb.y, across)
    y_relay = relay(ty, y_far)
    a_own = (spread(ta, yh, x, right), spread(ta, yh, x, left))
    a_up.wait_recv()
    a_oth = (spread(ta, yo, x, right), spread(ta, yo, x, left))
    hand(ta, yo, x)
    settle(ty, y_near, y_relay)
    y_norm = finish(ty)
    b_y.wait_recv()
    b_norm = finish(tb, (tb.y,))

    def received(t, copy, y, xx):
        copy.wait_recv()
        hand(t, y, xx)

    received(ta, a_own[0], yh, xl)
    a_fwd0 = spread(ta, yh, xl, right)
    received(ta, a_own[1], yh, xr)
    received(ta, a_oth[1], yo, xr)
    a_fwd1 = spread(ta, yo, xr, left)
    received(ta, a_oth[0], yo, xl)

    update(ty, y_norm)
    y_own = (spread(ty, yh, x, right), spread(ty, yh, x, left))
    y_up = [spread(ty, yh, x, across)]
    hand(ty, yh, x)
    update(tb, b_norm)
    b_up = spread(tb, yh, x, across)
    b_own = (spread(tb, yh, x, right), spread(tb, yh, x, left))
    hand(tb, yh, x)
    received(ta, a_fwd0, yh, x2)
    received(ta, a_fwd1, yo, x2)

    y_own[0].wait_recv()
    part = ty.part(ty.half, owner(yh, xl, core), 0)
    y_fwd0 = net.start(part, part, right)
    y_up.append(spread(ty, yh, xl, across))
    y_own[1].wait_recv()
    part = ty.part(ty.half, owner(yh, xr, core), 1)
    y_fwd1 = net.start(part, part, left)
    y_up.append(spread(ty, yh, xr, across))
    b_up.wait_recv()
    b_oth = (spread(tb, yo, x, right), spread(tb, yo, x, left))
    hand(tb, yo, x)
    hand(ty, yh, xl)
    hand(ty, yh, xr)
    received(tb, b_own[0], yh, xl)
    b_fwd0 = spread(tb, yh, xl, right)
    received(tb, b_own[1], yh, xr)
    received(ty, y_up[0], yo, x)
    y_fwd0.wait_recv()
    y_fwd1.wait_recv()
    y_up.append(spread(ty, yh, x2, across))
    hand(ty, yh, x2)
    received(tb, b_oth[1], yo, xr)
    b_fwd1 = spread(tb, yo, xr, left)
    received(tb, b_oth[0], yo, xl)
    received(ty, y_up[1], yo, xl)
    received(ty, y_up[2], yo, xr)

    for copy in gathered:
        copy.wait_recv()
    for i in range(replicas):
        hn[i : i + 1, :] = nn_dst[i, 0:1, :]

    received(ty, y_up[3], yo, x2)
    received(tb, b_fwd0, yh, x2)
    received(tb, b_fwd1, yo, x2)
    for copy in handed:
        copy.wait_recv()
    net.drain()


def body(sg, su, sd, sn, pg, pu, pd, pn):
    replicas, models = lax.axis_size("replica"), lax.axis_size("model")
    width, cols = sg.shape[1:]
    f32, bf16 = jnp.float32, jnp.bfloat16

    def scratch(block, x_first):
        item = block if x_first else (block[0] // 2, block[1])
        return [
            pltpu.VMEM((2, XS, *block), f32),
            pltpu.VMEM((2, XS, *block), f32),
            pltpu.VMEM((2, *item), f32),
            pltpu.VMEM((2, *item), f32),
            pltpu.VMEM((2, *item), f32),
            pltpu.VMEM(block if x_first else (XS, *block), f32),
            pltpu.VMEM(block, f32),
            pltpu.VMEM((2, ROWS), f32),
            pltpu.VMEM((models, 2, ROWS), f32),
        ]

    vmem = pl.BlockSpec(memory_space=pltpu.VMEM)
    hbm = pl.BlockSpec(memory_space=pltpu.HBM)
    shape = jax.ShapeDtypeStruct
    out = pl.pallas_call(
        functools.partial(kernel, replicas, models),
        out_shape=(
            shape((width, cols), bf16),
            shape((width, cols), bf16),
            shape((cols, width), bf16),
            shape((replicas, ROWS), f32),
            shape((ROWS, cols), f32),
            shape((ROWS, cols), f32),
            shape((cols, ROWS), f32),
            shape((1, ROWS), f32),
        ),
        in_specs=[hbm, hbm, hbm, vmem, hbm, hbm, hbm, vmem],
        out_specs=(vmem,) * 8,
        scratch_shapes=[
            *scratch((ROWS, cols), True),
            *scratch((ROWS, cols), False),
            *scratch((cols, ROWS), True),
            pltpu.VMEM((replicas, 8, ROWS), f32),
            pltpu.VMEM((replicas, 8, ROWS), f32),
            pltpu.VMEM((8, ROWS), f32),
            pltpu.VMEM((replicas, 8, ROWS), f32),
            pltpu.SemaphoreType.DMA((27,)),
            pltpu.SemaphoreType.DMA((176,)),
            pltpu.SemaphoreType.DMA((176,)),
        ],
        compiler_params=pltpu.CompilerParams(
            collective_id=0, has_side_effects=True, vmem_limit_bytes=32 << 20
        ),
    )(sg, su, sd, sn, pg, pu, pd, pn.reshape(1, ROWS))
    hg, hu, hd, hn, ng, nu, nd, nn = out
    return hg, hu, hd, hn.reshape(-1).astype(bf16), ng, nu, nd, nn.reshape(ROWS)


def solution(mesh):
    return jax.shard_map(
        body,
        mesh=mesh,
        in_specs=(
            P("replica", None, "model"),
            P("replica", None, "model"),
            P("replica", "model", None),
            P("replica", None),
            P("replica", "model"),
            P("replica", "model"),
            P("model", "replica"),
            P("replica"),
        ),
        out_specs=(
            P(None, "model"),
            P(None, "model"),
            P("model", None),
            P(),
            P("replica", "model"),
            P("replica", "model"),
            P("model", "replica"),
            P("replica"),
        ),
        check_vma=False,
    )
```

```python
import functools

import jax
import jax.numpy as jnp
from jax import lax
from jax.experimental import pallas as pl
from jax.experimental.pallas import tpu as pltpu
from jax.sharding import PartitionSpec as P

MESH = pl.DeviceIdType.MESH
LEARN_RATE = 0.5
EPS = 1e-06
ROWS = 128
XS = 4


class Copies:
    def __init__(self, send, recv):
        self.send, self.recv, self.used, self.started = send, recv, 0, []

    def start(self, src, dst, target):
        copy = pltpu.make_async_remote_copy(
            src_ref=src,
            dst_ref=dst,
            send_sem=self.send.at[self.used],
            recv_sem=self.recv.at[self.used],
            device_id=target,
            device_id_type=MESH,
        )
        copy.start()
        self.used += 1
        self.started.append(copy)
        return copy

    def drain(self):
        for copy in self.started:
            copy.wait_send()


class Tensor:
    def __init__(self, by_rows, x_first, slope, param, half, new, scratch):
        self.by_rows, self.x_first = by_rows, x_first
        self.slope, self.param, self.half, self.new = slope, param, half, new
        (self.s, self.r, self.f, self.d, self.a, self.y, self.p, self.src, self.nm) = scratch
        self.block = self.p.shape

    def share(self, ref, index):
        at = pl.ds(pl.multiple_of(index * ROWS, ROWS), ROWS)
        return ref.at[at, :] if self.by_rows else ref.at[:, at]

    def part(self, ref, index, h):
        size = self.block[0] // 2
        if self.by_rows:
            return ref.at[pl.ds(pl.multiple_of(index * ROWS + h * size, size), size), :]
        return ref.at[pl.ds(h * size, size), pl.ds(pl.multiple_of(index * ROWS, ROWS), ROWS)]

    def item(self, yh, h, x):
        if self.x_first:
            return self.s.at[h, x]
        size = self.block[0] // 2
        return self.s.at[yh, x, pl.ds(h * size, size), :]

    def squares(self, value):
        value = value * value
        if not self.by_rows:
            return jnp.sum(value, axis=0, keepdims=True)
        folded = value[:, :ROWS]
        for at in range(ROWS, value.shape[1], ROWS):
            folded = folded + value[:, at : at + ROWS]
        return jnp.sum(folded.T, axis=0, keepdims=True)


def add(into, *others):
    value = into[...]
    for other in others:
        value = value + other[...]
    into[...] = value


def kernel(replicas, models, *refs):
    (sg, su, sd, sn, pg, pu, pd, pn), refs = refs[:8], refs[8:]
    (hg, hu, hd, hn, ng, nu, nd, nn), refs = refs[:8], refs[8:]
    ta, refs = Tensor(True, True, sg, pg, hg, ng, refs[:9]), refs[9:]
    ty, refs = Tensor(True, False, su, pu, hu, nu, refs[:9]), refs[9:]
    tb, refs = Tensor(False, True, sd, pd, hd, nd, refs[:9]), refs[9:]
    nv_src, nv_dst, nn_src, nn_dst, pn_here, sn_here, local_sem, send_sem, recv_sem = refs

    r = lax.axis_index("replica")
    m = lax.axis_index("model")
    core = r % 2
    x = (r // 2) % XS
    yh = r // (2 * XS)
    yo = 1 - yh
    xr, xl, x2 = (x + 1) % XS, (x + XS - 1) % XS, (x + 2) % XS

    def owner(y, xx, c):
        return (y * XS + xx) * 2 + c

    def device(y, xx, c):
        return {"replica": owner(y, xx, c), "model": m}

    right, left = device(yh, xr, core), device(yh, xl, core)
    across, partner = device(yo, x, core), device(yh, x, 1 - core)
    net = Copies(send_sem, recv_sem)

    order = [(ta, 0, x2), (ta, 1, x2), (ty, yo, x2), (ta, 1, xr), (ta, 0, xl), (ty, yo, xr)]
    order += [(ta, 0, xr), (ta, 1, xl), (ty, yo, xl), (tb, 0, x2), (tb, 1, x2)]
    order += [(ty, yh, x2), (ty, yh, xr), (ta, yo, x), (ta, yh, x), (tb, 1, xr), (tb, 0, xl)]
    order += [(ty, yh, xl), (ty, yo, x), (tb, 0, xr), (tb, 1, xl), (ty, yh, x)]
    order += [(tb, yo, x), (tb, yh, x)]
    loads = []
    for i, (t, y, xx) in enumerate(order):
        copy = pltpu.make_async_copy(
            t.share(t.slope.at[0], owner(y, xx, core)), t.s.at[y, xx], local_sem.at[i]
        )
        copy.start()
        loads.append(copy)
    params = []
    for i, t in enumerate((ta, ty, tb)):
        copy = pltpu.make_async_copy(t.param, t.p, local_sem.at[len(order) + i])
        copy.start()
        params.append(copy)
    copy = pltpu.make_async_copy(pn, pn_here, local_sem.at[27])
    copy.start()
    params.append(copy)
    small = pltpu.make_async_copy(sn, sn_here, local_sem.at[28])
    small.start()

    barrier = pltpu.get_barrier_semaphore()
    peers = [{"replica": (r + k) % replicas, "model": m} for k in range(1, replicas)]
    others = [{"replica": r, "model": (m + k) % models} for k in range(1, models)]
    for peer in peers + others:
        pl.semaphore_signal(barrier, inc=1, device_id=peer, device_id_type=MESH)
    small.wait()
    for i in range(replicas):
        nv_src[i, 0:1, :] = sn_here[0:1, i * ROWS : (i + 1) * ROWS]
    pl.semaphore_wait(barrier, replicas + models - 2)

    swaps = []
    for t, y, xx in order:
        swaps.append(
            net.start(t.share(t.slope.at[0], owner(y, xx, 1 - core)), t.r.at[y, xx], partner)
        )
    vectors = []
    for k, peer in enumerate(peers, 1):
        vectors.append(
            net.start(nv_src.at[peer["replica"], pl.ds(0, 1)], nv_dst.at[k, pl.ds(0, 1)], peer)
        )

    taken = [0]

    def take(count):
        for i in range(taken[0], taken[0] + count):
            t, y, xx = order[i]
            loads[i].wait()
            swaps[i].wait_recv()
            add(t.s.at[y, xx], t.r.at[y, xx])
        taken[0] += count

    def far(t):
        return (
            net.start(t.item(yh, 0, x2), t.f.at[0], right),
            net.start(t.item(yh, 1, x2), t.f.at[1], left),
        )

    def near(t):
        return (
            net.start(t.item(yh, 0, xl), t.d.at[0], left),
            net.start(t.item(yh, 1, xr), t.d.at[1], right),
        )

    def relay(t, got):
        got[0].wait_recv()
        add(t.item(yh, 0, xr), t.f.at[0])
        first = net.start(t.item(yh, 0, xr), t.a.at[0], right)
        got[1].wait_recv()
        add(t.item(yh, 1, xl), t.f.at[1])
        return first, net.start(t.item(yh, 1, xl), t.a.at[1], left)

    def settle(t, direct, relayed):
        for h in (0, 1):
            direct[h].wait_recv()
        for h in (0, 1):
            relayed[h].wait_recv()
            add(t.item(yh, h, x), t.d.at[h], t.a.at[h])

    def finish(t, extra=()):
        own = t.s.at[yh, x]
        value = own[...]
        for e in extra:
            value = value + e[...]
        value = value * (replicas**-0.5)
        own[...] = value
        t.src[0:1, :] = t.squares(value)
        sent = [
            net.start(t.src, t.nm.at[k], peer) for k, peer in enumerate(others, 1)
        ]
        return sent

    def update(t, sent):
        total = t.src[...]
        for copy in sent:
            copy.wait_recv()
        for k in range(1, models):
            total = total + t.nm[k]
        ratio = jnp.sqrt(total[1:2]) * lax.rsqrt(total[0:1] + EPS)
        if t.by_rows:
            ratio = jnp.broadcast_to(ratio, (ROWS, ROWS)).T
            ratio = jnp.concatenate([ratio] * (t.block[1] // ROWS), axis=1)
        new = t.p[...] - LEARN_RATE * (t.s[yh, x] * ratio)
        t.new[...] = new
        t.share(t.half, owner(yh, x, core))[...] = new.astype(jnp.bfloat16)

    def blk(t, y, xx):
        return t.share(t.half, owner(y, xx, core))

    def spread(t, y, xx, target):
        return net.start(blk(t, y, xx), blk(t, y, xx), target)

    handed = []

    def hand(t, y, xx):
        handed.append(spread(t, y, xx, partner))

    take(2)
    a_far = far(ta)
    take(1)
    y_got = [net.start(ty.s.at[yo, x2], ty.y.at[0], across)]
    take(2)
    a_near = near(ta)
    take(1)
    y_got.append(net.start(ty.s.at[yo, xr], ty.y.at[1], across))
    take(3)
    y_got.append(net.start(ty.s.at[yo, xl], ty.y.at[2], across))
    take(2)
    for t, copy in zip((ta, ty, tb), params):
        copy.wait()
        t.src[1:2, :] = t.squares(t.p[...])
    take(2)
    a_relay = relay(ta, a_far)
    b_far = far(tb)
    take(4)
    b_near = near(tb)
    take(7)

    mean = nv_src[r, 0:1, :]
    for k, copy in enumerate(vectors, 1):
        copy.wait_recv()
        mean = mean + nv_dst[k, 0:1, :]
    params[3].wait()
    new = pn_here[...] - LEARN_RATE * (mean * (replicas**-0.5))
    nn[...] = new
    nn_src[0:1, :] = new
    nn_dst[r, 0:1, :] = new
    gathered = [
        net.start(nn_src.at[pl.ds(0, 1)], nn_dst.at[r, pl.ds(0, 1)], peer) for peer in peers
    ]

    y_got[0].wait_recv()
    add(ty.s.at[yh, x2], ty.y.at[0])
    y_got[1].wait_recv()
    add(ty.s.at[yh, xr], ty.y.at[1])
    settle(ta, a_near, a_relay)
    a_y = net.start(ta.s.at[yo, x], ta.y, across)
    y_got.append(net.start(ty.s.at[yo, x], ty.y.at[3], across))
    y_got[2].wait_recv()
    add(ty.s.at[yh, xl], ty.y.at[2])
    b_relay = relay(tb, b_far)
    y_far = far(ty)
    y_near = near(ty)
    a_y.wait_recv()
    a_norm = finish(ta, (ta.y,))
    y_got[3].wait_recv()
    add(ty.s.at[yh, x], ty.y.at[3])
    update(ta, a_norm)
    a_up = spread(ta, yh, x, across)
    hand(ta, yh, x)
    settle(tb, b_near, b_relay)
    b_y = net.start(tb.s.at[yo, x], tb.y, across)
    y_relay = relay(ty, y_far)
    a_own = (spread(ta, yh, x, right), spread(ta, yh, x, left))
    a_up.wait_recv()
    a_oth = (spread(ta, yo, x, right), spread(ta, yo, x, left))
    hand(ta, yo, x)
    settle(ty, y_near, y_relay)
    y_norm = finish(ty)
    b_y.wait_recv()
    b_norm = finish(tb, (tb.y,))

    def received(t, copy, y, xx):
        copy.wait_recv()
        hand(t, y, xx)

    received(ta, a_own[0], yh, xl)
    a_fwd0 = spread(ta, yh, xl, right)
    received(ta, a_own[1], yh, xr)
    received(ta, a_oth[1], yo, xr)
    a_fwd1 = spread(ta, yo, xr, left)
    received(ta, a_oth[0], yo, xl)

    update(ty, y_norm)
    y_own = (spread(ty, yh, x, right), spread(ty, yh, x, left))
    y_up = [spread(ty, yh, x, across)]
    hand(ty, yh, x)
    update(tb, b_norm)
    b_up = spread(tb, yh, x, across)
    b_own = (spread(tb, yh, x, right), spread(tb, yh, x, left))
    hand(tb, yh, x)
    received(ta, a_fwd0, yh, x2)
    received(ta, a_fwd1, yo, x2)

    y_own[0].wait_recv()
    part = ty.part(ty.half, owner(yh, xl, core), 0)
    y_fwd0 = net.start(part, part, right)
    y_up.append(spread(ty, yh, xl, across))
    y_own[1].wait_recv()
    part = ty.part(ty.half, owner(yh, xr, core), 1)
    y_fwd1 = net.start(part, part, left)
    y_up.append(spread(ty, yh, xr, across))
    b_up.wait_recv()
    b_oth = (spread(tb, yo, x, right), spread(tb, yo, x, left))
    hand(tb, yo, x)
    hand(ty, yh, xl)
    hand(ty, yh, xr)
    received(tb, b_own[0], yh, xl)
    b_fwd0 = spread(tb, yh, xl, right)
    received(tb, b_own[1], yh, xr)
    received(ty, y_up[0], yo, x)
    y_fwd0.wait_recv()
    y_fwd1.wait_recv()
    y_up.append(spread(ty, yh, x2, across))
    hand(ty, yh, x2)
    received(tb, b_oth[1], yo, xr)
    b_fwd1 = spread(tb, yo, xr, left)
    received(tb, b_oth[0], yo, xl)
    received(ty, y_up[1], yo, xl)
    received(ty, y_up[2], yo, xr)

    for copy in gathered:
        copy.wait_recv()
    for i in range(replicas):
        hn[i * ROWS : (i + 1) * ROWS] = nn_dst[i, 0, :].astype(jnp.bfloat16)

    received(ty, y_up[3], yo, x2)
    received(tb, b_fwd0, yh, x2)
    received(tb, b_fwd1, yo, x2)
    for copy in handed:
        copy.wait_recv()
    net.drain()


def store(*refs):
    copies = [
        pltpu.make_async_copy(refs[i], refs[8 + i], refs[16].at[i]) for i in range(8)
    ]
    for copy in copies:
        copy.start()
    for copy in copies:
        copy.wait()


def body(sg, su, sd, sn, pg, pu, pd, pn):
    arrays = (sg, su, sd, sn, pg, pu, pd, pn.reshape(1, ROWS))
    replicas, models = lax.axis_size("replica"), lax.axis_size("model")
    width, cols = sg.shape[1:]
    f32, bf16 = jnp.float32, jnp.bfloat16

    def scratch(block, x_first):
        item = block if x_first else (block[0] // 2, block[1])
        return [
            pltpu.VMEM((2, XS, *block), f32),
            pltpu.VMEM((2, XS, *block), f32),
            pltpu.VMEM((2, *item), f32),
            pltpu.VMEM((2, *item), f32),
            pltpu.VMEM((2, *item), f32),
            pltpu.VMEM(block if x_first else (XS, *block), f32),
            pltpu.VMEM(block, f32),
            pltpu.VMEM((2, ROWS), f32),
            pltpu.VMEM((models, 2, ROWS), f32),
        ]

    vmem = pl.BlockSpec(memory_space=pltpu.VMEM)
    hbm = pl.BlockSpec(memory_space=pltpu.HBM)
    shape = jax.ShapeDtypeStruct
    out = pl.pallas_call(
        functools.partial(kernel, replicas, models),
        out_shape=(
            shape((width, cols), bf16),
            shape((width, cols), bf16),
            shape((cols, width), bf16),
            shape((width,), bf16),
            shape((ROWS, cols), f32),
            shape((ROWS, cols), f32),
            shape((cols, ROWS), f32),
            shape((1, ROWS), f32),
        ),
        in_specs=[hbm] * 8,
        out_specs=(vmem,) * 8,
        scratch_shapes=[
            *scratch((ROWS, cols), True),
            *scratch((ROWS, cols), False),
            *scratch((cols, ROWS), True),
            pltpu.VMEM((replicas, 8, ROWS), f32),
            pltpu.VMEM((replicas, 8, ROWS), f32),
            pltpu.VMEM((8, ROWS), f32),
            pltpu.VMEM((replicas, 8, ROWS), f32),
            pltpu.VMEM((1, ROWS), f32),
            pltpu.VMEM((1, width), f32),
            pltpu.SemaphoreType.DMA((29,)),
            pltpu.SemaphoreType.DMA((176,)),
            pltpu.SemaphoreType.DMA((176,)),
        ],
        compiler_params=pltpu.CompilerParams(
            collective_id=0, has_side_effects=True, vmem_limit_bytes=32 << 20
        ),
    )(*(pltpu.with_memory_space_constraint(a, pltpu.HBM) for a in arrays))
    out = (*out[:3], out[3].reshape(width), *out[4:])
    out = pl.pallas_call(
        store,
        out_shape=tuple(shape(o.shape, o.dtype) for o in out),
        in_specs=[vmem] * 8,
        out_specs=(hbm,) * 8,
        scratch_shapes=[pltpu.SemaphoreType.DMA((8,))],
        compiler_params=pltpu.CompilerParams(vmem_limit_bytes=8 << 20),
    )(*(pltpu.with_memory_space_constraint(o, pltpu.VMEM) for o in out))
    return (*out[:7], out[7].reshape(ROWS))


def solution(mesh):
    return jax.shard_map(
        body,
        mesh=mesh,
        in_specs=(
            P("replica", None, "model"),
            P("replica", None, "model"),
            P("replica", "model", None),
            P("replica", None),
            P("replica", "model"),
            P("replica", "model"),
            P("model", "replica"),
            P("replica"),
        ),
        out_specs=(
            P(None, "model"),
            P(None, "model"),
            P("model", None),
            P(),
            P("replica", "model"),
            P("replica", "model"),
            P("model", "replica"),
            P("replica"),
        ),
        check_vma=False,
    )
```

```python
import functools

import jax
import jax.numpy as jnp
from jax import lax
from jax.experimental import pallas as pl
from jax.experimental.pallas import tpu as pltpu
from jax.sharding import PartitionSpec as P

MESH = pl.DeviceIdType.MESH
LEARN_RATE = 0.5
EPS = 1e-06
ROWS = 128
XS = 4


class Copies:
    def __init__(self, send, recv):
        self.send, self.recv, self.used, self.started = send, recv, 0, []
        self.drained = 0

    def start(self, src, dst, target):
        copy = pltpu.make_async_remote_copy(
            src_ref=src,
            dst_ref=dst,
            send_sem=self.send.at[self.used],
            recv_sem=self.recv.at[self.used],
            device_id=target,
            device_id_type=MESH,
        )
        copy.start()
        self.used += 1
        self.started.append(copy)
        return copy

    def mark(self):
        return len(self.started)

    def drain(self, upto):
        for copy in self.started[self.drained : upto]:
            copy.wait_send()
        self.drained = max(self.drained, upto)


class Matrix:
    def __init__(self, by_rows, slope, param, half, new, s, r, p):
        self.by_rows, self.slope, self.param, self.half, self.new = by_rows, slope, param, half, new
        self.s, self.r, self.p = s, r, p

    def share(self, ref, index):
        at = pl.ds(pl.multiple_of(index * ROWS, ROWS), ROWS)
        return ref.at[at, :] if self.by_rows else ref.at[:, at]


class Tensor:
    def __init__(self, whole, x_first, low, rows, f, d, a, y, src, nm):
        self.whole, self.x_first, self.low, self.rows = whole, x_first, low, rows
        self.f, self.d, self.a, self.y, self.src, self.nm = f, d, a, y, src, nm
        self.by_rows = whole.by_rows
        self.p = whole.p.at[pl.ds(low, rows)]
        self.new = whole.new.at[pl.ds(low, rows)]

    def sums(self, y, x):
        return self.whole.s.at[y, x, pl.ds(self.low, self.rows)]

    def block(self, index):
        return self.part(index, 0, self.rows)

    def part(self, index, at, rows):
        at = self.low + at
        if self.by_rows:
            at = pl.ds(pl.multiple_of(index * ROWS + at, rows), rows)
            return self.whole.half.at[at, :]
        return self.whole.half.at[pl.ds(at, rows), pl.ds(pl.multiple_of(index * ROWS, ROWS), ROWS)]

    def item(self, yh, h, x):
        if self.x_first:
            return self.sums(h, x)
        size = self.rows // 2
        return self.whole.s.at[yh, x, pl.ds(self.low + h * size, size)]

    def squares(self, value):
        value = value * value
        if not self.by_rows:
            return jnp.sum(value, axis=0, keepdims=True)
        folded = value[:, :ROWS]
        for at in range(ROWS, value.shape[1], ROWS):
            folded = folded + value[:, at : at + ROWS]
        if self.rows < ROWS:
            folded = jnp.concatenate([folded, jnp.zeros_like(folded)], axis=0)
        return jnp.sum(folded.T, axis=0, keepdims=True)


class Vector:
    x_first = True

    def __init__(self, s, f, d, a, y):
        self.s, self.f, self.d, self.a, self.y = s, f, d, a, y

    def item(self, yh, h, x):
        return self.s.at[h, x]


def add(into, *others):
    value = into[...]
    for other in others:
        value = value + other[...]
    into[...] = value


def kernel(replicas, models, *refs):
    (sg, su, sd, sn, pg, pu, pd, pn), refs = refs[:8], refs[8:]
    (hg, hu, hd, hn, ng, nu, nd, nn), refs = refs[:8], refs[8:]
    my, refs = Matrix(True, sg, pg, hg, ng, *refs[:3]), refs[3:]
    mb, refs = Matrix(True, su, pu, hu, nu, *refs[:3]), refs[3:]
    ma, refs = Matrix(False, sd, pd, hd, nd, *refs[:3]), refs[3:]
    half = ROWS // 2
    ta, refs = Tensor(ma, True, 0, ma.p.shape[0], *refs[:6]), refs[6:]
    b1, refs = Tensor(mb, True, 0, half, *refs[:6]), refs[6:]
    b2, refs = Tensor(mb, True, half, half, *refs[:6]), refs[6:]
    y1, refs = Tensor(my, False, 0, half, *refs[:3], None, *refs[3:5]), refs[5:]
    y2, refs = Tensor(my, False, half, half, *refs[:3], None, *refs[3:5]), refs[5:]
    y_in, refs = refs[0], refs[1:]
    tn, refs = Vector(*refs[:5]), refs[5:]
    gain, pn_here, sn_here, sn_other, local_sem, send_sem, recv_sem, hop_sem = refs

    r = lax.axis_index("replica")
    m = lax.axis_index("model")
    core = r % 2
    x = (r // 2) % XS
    yh = r // (2 * XS)
    yo = 1 - yh
    xr, xl, x2 = (x + 1) % XS, (x + XS - 1) % XS, (x + 2) % XS

    def owner(y, xx, c):
        return (y * XS + xx) * 2 + c

    def device(y, xx, c):
        return {"replica": owner(y, xx, c), "model": m}

    right, left = device(yh, xr, core), device(yh, xl, core)
    across, partner = device(yo, x, core), device(yh, x, 1 - core)
    net = Copies(send_sem, recv_sem)
    others = [{"replica": r, "model": (m + k) % models} for k in range(1, models)]
    zs = models // 2
    z, yl = m // 2, m % 2
    up = {"replica": r, "model": (z + 1) % zs * 2 + yl}
    down = {"replica": r, "model": (z + zs - 1) % zs * 2 + yl}
    beside = {"replica": r, "model": z * 2 + 1 - yl}

    def signal(sem, *peers):
        for peer in peers:
            pl.semaphore_signal(sem, inc=1, device_id=peer, device_id_type=MESH)

    barrier = pltpu.get_barrier_semaphore()
    signal(barrier, partner, right, left, across, up, down, beside)

    order = [("af", ma, 0, x2), ("af", ma, 1, x2), ("y0", my, yo, x2)]
    order += [("an", ma, 1, xr), ("an", ma, 0, xl), ("y1", my, yo, xr)]
    order += [("ar", ma, 0, xr), ("ar", ma, 1, xl), ("y2", my, yo, xl)]
    order += [("bf", mb, 0, x2), ("bf", mb, 1, x2), ("y3", my, yo, x)]
    order += [("yx2", my, yh, x2), ("bn", mb, 1, xr), ("bn", mb, 0, xl)]
    order += [("br", mb, 0, xr), ("br", mb, 1, xl), ("yx", my, yh, xr)]
    order += [("yx", my, yh, xl), ("ao", ma, 0, x), ("ao", ma, 1, x)]
    order += [("bo", mb, 0, x), ("bo", mb, 1, x), ("yo", my, yh, x)]
    loads = []
    for i, (_, t, y, xx) in enumerate(order):
        copy = pltpu.make_async_copy(
            t.share(t.slope.at[0], owner(y, xx, core)), t.s.at[y, xx], local_sem.at[i]
        )
        copy.start()
        loads.append(copy)
    params = []
    for i, t in enumerate((ma, mb, my)):
        copy = pltpu.make_async_copy(t.param, t.p, local_sem.at[len(order) + i])
        copy.start()
        params.append(copy)
    copy = pltpu.make_async_copy(pn, pn_here, local_sem.at[27])
    copy.start()
    params.append(copy)
    small = pltpu.make_async_copy(sn, sn_here, local_sem.at[28])
    small.start()
    pl.semaphore_wait(barrier, 7)

    swaps = []
    for tag, t, y, xx in order:
        swaps.append(
            net.start(t.share(t.slope.at[0], owner(y, xx, 1 - core)), t.r.at[y, xx], partner)
        )
        if tag == "y2":
            small_swap = net.start(sn, sn_other, partner)
            signal(hop_sem.at[0], up, down)
    swapped = net.mark()

    taken = [0]

    def take(tag):
        end = max(i for i, entry in enumerate(order) if entry[0] == tag) + 1
        for i in range(taken[0], end):
            _, t, y, xx = order[i]
            loads[i].wait()
            swaps[i].wait_recv()
            add(t.s.at[y, xx], t.r.at[y, xx])
        taken[0] = max(taken[0], end)

    def far(t):
        return (
            net.start(t.item(yh, 0, x2), t.f.at[0], right),
            net.start(t.item(yh, 1, x2), t.f.at[1], left),
        )

    def near(t):
        return (
            net.start(t.item(yh, 0, xl), t.d.at[0], left),
            net.start(t.item(yh, 1, xr), t.d.at[1], right),
        )

    def relay(t, got):
        got[0].wait_recv()
        add(t.item(yh, 0, xr), t.f.at[0])
        first = net.start(t.item(yh, 0, xr), t.a.at[0], right)
        got[1].wait_recv()
        add(t.item(yh, 1, xl), t.f.at[1])
        return first, net.start(t.item(yh, 1, xl), t.a.at[1], left)

    def settle(t, direct, relayed):
        for h in (0, 1):
            direct[h].wait_recv()
        for h in (0, 1):
            relayed[h].wait_recv()
            add(t.item(yh, h, x), t.d.at[h], t.a.at[h])

    def finish(t, extra=()):
        own = t.sums(yh, x)
        value = own[...]
        for e in extra:
            value = value + e[...]
        value = value * (replicas**-0.5)
        own[...] = value
        t.src[0:1, :] = t.squares(value)
        return [net.start(t.src, t.nm.at[k], peer) for k, peer in enumerate(others, 1)]

    def update(t, sent):
        total = t.src[...]
        for copy in sent:
            copy.wait_recv()
        for k in range(1, models):
            total = total + t.nm[k]
        ratio = jnp.sqrt(total[1:2]) * lax.rsqrt(total[0:1] + EPS)
        if t.by_rows:
            ratio = jnp.broadcast_to(ratio, (ROWS, ROWS)).T[: t.rows]
            ratio = jnp.concatenate([ratio] * (t.p.shape[1] // ROWS), axis=1)
        new = t.p[...] - LEARN_RATE * (t.sums(yh, x)[...] * ratio)
        t.new[...] = new
        t.block(owner(yh, x, core))[...] = new.astype(jnp.bfloat16)

    def spread(t, y, xx, target):
        block = t.block(owner(y, xx, core))
        return net.start(block, block, target)

    handed = []

    def hand(t, y, xx):
        handed.append(spread(t, y, xx, partner))

    def received(t, copy, y, xx):
        copy.wait_recv()
        hand(t, y, xx)

    def both(t, y):
        return spread(t, y, x, right), spread(t, y, x, left)

    def fold(got, xx, j):
        got.wait_recv()
        add(my.s.at[yh, xx], y_in.at[j])

    take("af")
    a_far = far(ta)
    take("y0")
    y_got = [net.start(my.s.at[yo, x2], y_in.at[0], across)]
    take("an")
    a_near = near(ta)
    take("y1")
    y_got.append(net.start(my.s.at[yo, xr], y_in.at[1], across))
    take("ar")
    take("y2")
    y_got.append(net.start(my.s.at[yo, xl], y_in.at[2], across))
    for copy in params[:3]:
        copy.wait()
    for t in (ta, b1, b2, y1, y2):
        t.src[1:2, :] = t.squares(t.p[...])
    small.wait()
    small_swap.wait_recv()
    for y in (0, 1):
        for xx in range(XS):
            at = pl.ds(pl.multiple_of(owner(y, xx, core) * ROWS, ROWS), ROWS)
            tn.s[y, xx] = sn_here[0:1, at] + sn_other[0:1, at]
    n_far = far(tn)
    n_near = near(tn)
    take("bf")
    pl.semaphore_wait(hop_sem.at[0], 2)
    signal(hop_sem.at[1], up, down)
    take("yx2")
    a_relay = relay(ta, a_far)
    take("bn")
    fold(y_got[0], x2, 0)
    pl.semaphore_wait(hop_sem.at[1], 2)
    signal(hop_sem.at[2], up, down)
    take("yo")
    n_relay = relay(tn, n_far)
    b1_far, b2_far = far(b1), far(b2)
    b1_near = near(b1)
    pl.semaphore_wait(hop_sem.at[2], 2)
    signal(hop_sem.at[3], beside)
    fold(y_got[1], xr, 1)
    net.drain(swapped)
    settle(ta, a_near, a_relay)
    a_y = net.start(ta.sums(yo, x), ta.y, across)
    y_got.append(net.start(my.s.at[yo, x], y_in.at[3], across))
    settle(tn, n_near, n_relay)
    n_y = net.start(tn.s.at[yo, x], tn.y, across)
    fold(y_got[2], xl, 2)
    b1_relay = relay(b1, b1_far)
    b2_near = near(b2)
    b2_relay = relay(b2, b2_far)
    y1_far, y2_far = far(y1), far(y2)
    y1_near, y2_near = near(y1), near(y2)
    pl.semaphore_wait(hop_sem.at[3], 1)
    mark = net.mark() - 16
    net.drain(mark)
    a_y.wait_recv()
    a_norm = finish(ta, (ta.y,))
    settle(b1, b1_near, b1_relay)
    b1_y = net.start(b1.sums(yo, x), b1.y, across)
    n_y.wait_recv()
    params[3].wait()
    add(tn.s.at[yh, x], tn.y)
    gain[core, yh * XS + x] = pn_here[...] - LEARN_RATE * (tn.s[yh, x] * (replicas**-0.5))
    nn[...] = gain[core, yh * XS + x]

    def tell(y, xx, target):
        row = gain.at[core, y * XS + xx]
        return net.start(row, row, target)

    n_up = tell(yh, x, across)
    fold(y_got[3], x, 3)
    update(ta, a_norm)
    a_up = spread(ta, yh, x, across)
    hand(ta, yh, x)
    settle(b2, b2_near, b2_relay)
    b2_y = net.start(b2.sums(yo, x), b2.y, across)
    y1_relay = relay(y1, y1_far)
    b1_y.wait_recv()
    b1_norm = finish(b1, (b1.y,))
    y2_relay = relay(y2, y2_far)
    n_own = (tell(yh, x, right), tell(yh, x, left))
    n_up.wait_recv()
    n_oth = (tell(yo, x, right), tell(yo, x, left))
    a_own = both(ta, yh)
    net.drain(net.mark() - 32)
    settle(y1, y1_near, y1_relay)
    y1_norm = finish(y1)
    a_up.wait_recv()
    a_oth = both(ta, yo)
    hand(ta, yo, x)
    b2_y.wait_recv()
    b2_norm = finish(b2, (b2.y,))
    update(b1, b1_norm)
    b1_up = spread(b1, yh, x, across)
    b1_own = both(b1, yh)
    hand(b1, yh, x)
    settle(y2, y2_near, y2_relay)
    y2_norm = finish(y2)
    n_own[0].wait_recv()
    n_fwd0 = tell(yh, xl, right)
    n_own[1].wait_recv()
    n_oth[0].wait_recv()
    n_oth[1].wait_recv()
    n_fwd1 = tell(yo, xr, left)
    received(ta, a_own[0], yh, xl)
    a_fwd0 = spread(ta, yh, xl, right)
    received(ta, a_own[1], yh, xr)
    update(y1, y1_norm)
    y1_own = both(y1, yh)
    y1_up = [spread(y1, yh, x, across)]
    hand(y1, yh, x)
    received(ta, a_oth[1], yo, xr)
    a_fwd1 = spread(ta, yo, xr, left)
    update(b2, b2_norm)
    b2_up = spread(b2, yh, x, across)
    update(y2, y2_norm)
    y2_own = both(y2, yh)
    b2_own = both(b2, yh)
    y2_up = [spread(y2, yh, x, across)]
    hand(b2, yh, x)
    hand(y2, yh, x)
    b1_up.wait_recv()
    b1_oth = both(b1, yo)
    received(ta, a_oth[0], yo, xl)
    hand(b1, yo, x)
    received(b1, b1_own[0], yh, xl)
    b1_fwd0 = spread(b1, yh, xl, right)
    received(b1, b1_own[1], yh, xr)
    n_fwd0.wait_recv()
    n_fwd1.wait_recv()
    n_hand = net.start(gain.at[core], gain.at[core], partner)
    net.drain(net.mark() - 32)

    def pass_on(t, own, ups):
        own[0].wait_recv()
        part = t.part(owner(yh, xl, core), 0, t.rows // 2)
        first = net.start(part, part, right)
        own[1].wait_recv()
        part = t.part(owner(yh, xr, core), t.rows // 2, t.rows // 2)
        second = net.start(part, part, left)
        ups.append(spread(t, yh, xl, across))
        ups.append(spread(t, yh, xr, across))
        hand(t, yh, xl)
        hand(t, yh, xr)
        return first, second

    def last_up(t, passed, ups):
        passed[0].wait_recv()
        passed[1].wait_recv()
        ups.append(spread(t, yh, x2, across))
        hand(t, yh, x2)

    y1_fwd = pass_on(y1, y1_own, y1_up)
    b2_up.wait_recv()
    b2_oth = both(b2, yo)
    hand(b2, yo, x)
    y2_fwd = pass_on(y2, y2_own, y2_up)
    received(b2, b2_own[0], yh, xl)
    b2_fwd0 = spread(b2, yh, xl, right)
    received(b2, b2_own[1], yh, xr)
    received(b1, b1_oth[1], yo, xr)
    b1_fwd1 = spread(b1, yo, xr, left)
    last_up(y1, y1_fwd, y1_up)
    received(b1, b1_oth[0], yo, xl)
    received(ta, a_fwd0, yh, x2)
    received(ta, a_fwd1, yo, x2)
    n_hand.wait_recv()
    for y in (0, 1):
        for xx in range(XS):
            for c in (0, 1):
                at = owner(y, xx, c) * ROWS
                hn[at : at + ROWS] = gain[c, y * XS + xx, 0, :].astype(jnp.bfloat16)
    received(b2, b2_oth[1], yo, xr)
    b2_fwd1 = spread(b2, yo, xr, left)
    last_up(y2, y2_fwd, y2_up)
    received(b2, b2_oth[0], yo, xl)
    received(y1, y1_up[0], yo, x)
    received(y2, y2_up[0], yo, x)
    received(b1, b1_fwd0, yh, x2)
    received(y1, y1_up[1], yo, xl)
    received(y1, y1_up[2], yo, xr)
    received(b1, b1_fwd1, yo, x2)
    early = len(handed) - 10
    for copy in handed[:early]:
        copy.wait_recv()
    net.drain(net.mark() - 16)
    received(y2, y2_up[1], yo, xl)
    received(y2, y2_up[2], yo, xr)
    received(b2, b2_fwd0, yh, x2)
    received(y1, y1_up[3], yo, x2)
    received(b2, b2_fwd1, yo, x2)
    received(y2, y2_up[3], yo, x2)
    for copy in handed[early:]:
        copy.wait_recv()
    net.drain(net.mark())


def store(*refs):
    copies = [
        pltpu.make_async_copy(refs[i], refs[8 + i], refs[16].at[i]) for i in range(8)
    ]
    for copy in copies:
        copy.start()
    for copy in copies:
        copy.wait()


def body(sg, su, sd, sn, pg, pu, pd, pn):
    arrays = (sg, su, sd, sn, pg, pu, pd, pn.reshape(1, ROWS))
    replicas, models = lax.axis_size("replica"), lax.axis_size("model")
    width, cols = sg.shape[1:]
    f32, bf16 = jnp.float32, jnp.bfloat16

    def matrix(share):
        sums = pltpu.VMEM((2, XS, *share), f32)
        return [sums, sums, pltpu.VMEM(share, f32)]

    def scratch(block, x_first):
        item = block if x_first else (block[0] // 2, block[1])
        arrived = [pltpu.VMEM((2, *item), f32)] * 3 + [pltpu.VMEM(block, f32)] * x_first
        return arrived + [pltpu.VMEM((2, ROWS), f32), pltpu.VMEM((models, 2, ROWS), f32)]

    vmem = pl.BlockSpec(memory_space=pltpu.VMEM)
    hbm = pl.BlockSpec(memory_space=pltpu.HBM)
    shape = jax.ShapeDtypeStruct
    out = pl.pallas_call(
        functools.partial(kernel, replicas, models),
        out_shape=(
            shape((width, cols), bf16),
            shape((width, cols), bf16),
            shape((cols, width), bf16),
            shape((width,), bf16),
            shape((ROWS, cols), f32),
            shape((ROWS, cols), f32),
            shape((cols, ROWS), f32),
            shape((1, ROWS), f32),
        ),
        in_specs=[hbm] * 8,
        out_specs=(vmem,) * 8,
        scratch_shapes=[
            *matrix((ROWS, cols)),
            *matrix((ROWS, cols)),
            *matrix((cols, ROWS)),
            *scratch((cols, ROWS), True),
            *scratch((ROWS // 2, cols), True),
            *scratch((ROWS // 2, cols), True),
            *scratch((ROWS // 2, cols), False),
            *scratch((ROWS // 2, cols), False),
            pltpu.VMEM((XS, ROWS, cols), f32),
            pltpu.VMEM((2, XS, 1, ROWS), f32),
            *[pltpu.VMEM((2, 1, ROWS), f32)] * 3,
            pltpu.VMEM((1, ROWS), f32),
            pltpu.VMEM((2, 2 * XS, 1, ROWS), f32),
            pltpu.VMEM((1, ROWS), f32),
            pltpu.VMEM((1, width), f32),
            pltpu.VMEM((1, width), f32),
            pltpu.SemaphoreType.DMA((29,)),
            pltpu.SemaphoreType.DMA((256,)),
            pltpu.SemaphoreType.DMA((256,)),
            pltpu.SemaphoreType.REGULAR((4,)),
        ],
        compiler_params=pltpu.CompilerParams(
            collective_id=0, has_side_effects=True, vmem_limit_bytes=32 << 20
        ),
    )(*(pltpu.with_memory_space_constraint(a, pltpu.HBM) for a in arrays))
    out = (*out[:3], out[3].reshape(width), *out[4:])
    out = pl.pallas_call(
        store,
        out_shape=tuple(shape(o.shape, o.dtype) for o in out),
        in_specs=[vmem] * 8,
        out_specs=(hbm,) * 8,
        scratch_shapes=[pltpu.SemaphoreType.DMA((8,))],
        compiler_params=pltpu.CompilerParams(vmem_limit_bytes=8 << 20),
    )(*(pltpu.with_memory_space_constraint(o, pltpu.VMEM) for o in out))
    return (*out[:7], out[7].reshape(ROWS))


def solution(mesh):
    return jax.shard_map(
        body,
        mesh=mesh,
        in_specs=(
            P("replica", None, "model"),
            P("replica", None, "model"),
            P("replica", "model", None),
            P("replica", None),
            P("replica", "model"),
            P("replica", "model"),
            P("model", "replica"),
            P("replica"),
        ),
        out_specs=(
            P(None, "model"),
            P(None, "model"),
            P("model", None),
            P(),
            P("replica", "model"),
            P("replica", "model"),
            P("model", "replica"),
            P("replica"),
        ),
        check_vma=False,
    )
```

```python
import functools

import jax
import jax.numpy as jnp
from jax import lax
from jax.experimental import pallas as pl
from jax.experimental.pallas import tpu as pltpu
from jax.sharding import PartitionSpec as P

MESH = pl.DeviceIdType.MESH
LEARN_RATE = 0.5
EPS = 1e-06
ROWS = 128
XS = 4
SENDS, RECVS = 34, 80


class Copies:
    def __init__(self, send, recv):
        self.send, self.recv, self.sends, self.recvs = send, recv, {}, {}

    def start(self, src, dst, target, sent, got):
        pltpu.make_async_remote_copy(
            src_ref=src,
            dst_ref=dst,
            send_sem=self.send.at[self.sends.setdefault(sent, len(self.sends))],
            recv_sem=self.recv.at[self.recvs.setdefault(got, len(self.recvs))],
            device_id=target,
            device_id_type=MESH,
        ).start()

    def gone(self, sent, size):
        pltpu.make_async_copy(size, size, self.send.at[self.sends[sent]]).wait()

    def here(self, got, size):
        pltpu.make_async_copy(size, size, self.recv.at[self.recvs[got]]).wait()


class Matrix:
    def __init__(self, by_rows, slope, param, half, new, s, r, p):
        self.by_rows, self.slope, self.param, self.half, self.new = by_rows, slope, param, half, new
        self.s, self.r, self.p = s, r, p

    def share(self, ref, index):
        at = pl.ds(pl.multiple_of(index * ROWS, ROWS), ROWS)
        return ref.at[at, :] if self.by_rows else ref.at[:, at]


class Tensor:
    def __init__(self, name, whole, x_first, direct, low, rows, x_in, y, src, nm):
        self.name, self.whole, self.x_first, self.direct = name, whole, x_first, direct
        self.low, self.rows, self.x_in, self.y, self.src, self.nm = low, rows, x_in, y, src, nm
        self.by_rows = whole.by_rows
        self.p = whole.p.at[pl.ds(low, rows)]
        self.new = whole.new.at[pl.ds(low, rows)]

    def blocks(self, count):
        if self.by_rows:
            return self.whole.half.at[pl.ds(0, count * self.rows), :]
        return self.whole.half.at[:, pl.ds(0, count * ROWS)]

    def sums(self, y, x):
        return self.whole.s.at[y, x, pl.ds(self.low, self.rows)]

    def block(self, index):
        return self.part(index, 0, self.rows)

    def part(self, index, at, rows):
        at = self.low + at
        if self.by_rows:
            at = pl.ds(pl.multiple_of(index * ROWS + at, rows), rows)
            return self.whole.half.at[at, :]
        return self.whole.half.at[pl.ds(at, rows), pl.ds(pl.multiple_of(index * ROWS, ROWS), ROWS)]

    def item(self, yh, h, x):
        if self.x_first:
            return self.sums(h, x)
        size = self.rows // 2
        return self.whole.s.at[yh, x, pl.ds(self.low + h * size, size)]

    def squares(self, value):
        value = value * value
        if not self.by_rows:
            return jnp.sum(value, axis=0, keepdims=True)
        folded = value[:, :ROWS]
        for at in range(ROWS, value.shape[1], ROWS):
            folded = folded + value[:, at : at + ROWS]
        if self.rows < ROWS:
            folded = jnp.concatenate([folded, jnp.zeros_like(folded)], axis=0)
        return jnp.sum(folded.T, axis=0, keepdims=True)


class Vector:
    name, x_first = "n", True

    def __init__(self, s, x_in, y):
        self.s, self.x_in, self.y = s, x_in, y

    def item(self, yh, h, x):
        return self.s.at[h, x]


def add(into, *others):
    value = into[...]
    for other in others:
        value = value + other[...]
    into[...] = value


def kernel(replicas, models, *refs):
    (sg, su, sd, sn, pg, pu, pd, pn), refs = refs[:8], refs[8:]
    (hg, hu, hd, hn, ng, nu, nd, nn), refs = refs[:8], refs[8:]
    my, refs = Matrix(True, sg, pg, hg, ng, *refs[:3]), refs[3:]
    mb, refs = Matrix(True, su, pu, hu, nu, *refs[:3]), refs[3:]
    ma, refs = Matrix(False, sd, pd, hd, nd, *refs[:3]), refs[3:]
    half = ROWS // 2
    deep = ma.p.shape[0]
    ta = Tensor("a", ma, True, False, 0, deep, None, None, *refs[2:4])
    a1 = Tensor("a1", ma, True, False, 0, deep // 2, *refs[:2], None, None)
    refs = refs[4:]
    a2 = Tensor("a2", ma, True, False, deep // 2, deep // 2, *refs[:2], None, None)
    refs = refs[2:]
    b1, refs = Tensor("b1", mb, True, False, 0, half, *refs[:4]), refs[4:]
    b2, refs = Tensor("b2", mb, True, False, half, half, *refs[:4]), refs[4:]
    y1, refs = Tensor("y1", my, False, True, 0, half, refs[0], None, *refs[1:3]), refs[3:]
    y2, refs = Tensor("y2", my, False, True, half, half, refs[0], None, *refs[1:3]), refs[3:]
    y_in, refs = refs[0], refs[1:]
    tn, refs = Vector(*refs[:3]), refs[3:]
    gain, pn_here, sn_here, sn_other, a_out, y_out, refs = *refs[:6], refs[6:]
    local_sem, send_sem, recv_sem, hop_sem = refs

    r = lax.axis_index("replica")
    m = lax.axis_index("model")
    core = r % 2
    x = (r // 2) % XS
    yh = r // (2 * XS)
    yo = 1 - yh
    xr, xl, x2 = (x + 1) % XS, (x + XS - 1) % XS, (x + 2) % XS

    def owner(y, xx, c):
        return (y * XS + xx) * 2 + c

    def device(y, xx, c):
        return {"replica": owner(y, xx, c), "model": m}

    right, left = device(yh, xr, core), device(yh, xl, core)
    across, partner = device(yo, x, core), device(yh, x, 1 - core)
    beyond = device(yh, x2, core)
    net = Copies(send_sem, recv_sem)
    others = [{"replica": r, "model": (m + k) % models} for k in range(1, models)]
    zs = models // 2
    z, yl = m // 2, m % 2
    up = {"replica": r, "model": (z + 1) % zs * 2 + yl}
    down = {"replica": r, "model": (z + zs - 1) % zs * 2 + yl}
    beside = {"replica": r, "model": z * 2 + 1 - yl}

    def signal(sem, *peers):
        for peer in peers:
            pl.semaphore_signal(sem, inc=1, device_id=peer, device_id_type=MESH)

    barrier = pltpu.get_barrier_semaphore()
    signal(barrier, partner, right, left, across, up, down, beside)

    order = [("af", ma, 0, x2), ("af", ma, 1, x2), ("y0", my, yo, x2)]
    order += [("an", ma, 1, xr), ("an", ma, 0, xl), ("y1", my, yo, xr)]
    order += [("ar", ma, 0, xr), ("ar", ma, 1, xl), ("y2", my, yo, xl)]
    order += [("bf", mb, 0, x2), ("bf", mb, 1, x2), ("y3", my, yo, x)]
    order += [("yx2", my, yh, x2), ("bn", mb, 1, xr), ("bn", mb, 0, xl)]
    order += [("br", mb, 0, xr), ("br", mb, 1, xl), ("yx", my, yh, xr)]
    order += [("yx", my, yh, xl), ("ao", ma, 0, x), ("ao", ma, 1, x)]
    order += [("bo", mb, 0, x), ("bo", mb, 1, x), ("yo", my, yh, x)]
    def load(src, dst, sem):
        pltpu.make_async_copy(src, dst, local_sem.at[sem]).start()

    def loaded(ref, sem):
        pltpu.make_async_copy(ref, ref, local_sem.at[sem]).wait()

    early, outs = {"af": ma, "an": ma, "y0": my}, {}
    for i, (tag, t, y, xx) in enumerate(order):
        if tag in early:
            n = len([k for k in outs if order[k][1] is t])
            outs[i] = (a_out if t is ma else y_out).at[n]
            load(t.share(t.slope.at[0], owner(y, xx, 1 - core)), outs[i], 0 if t is ma else 1)
    for tag, t, y, xx in order:
        load(t.share(t.slope.at[0], owner(y, xx, core)), t.s.at[y, xx], (ma, my, mb).index(t) + 2)
    for i, t in enumerate((ma, mb, my)):
        load(t.param, t.p, 5 + i)
    load(pn, pn_here, 8)
    load(sn, sn_here, 9)
    loaded(a_out, 0)
    loaded(y_out, 1)
    pl.semaphore_wait(barrier, 7)

    for i, (tag, t, y, xx) in enumerate(order):
        src = outs[i] if i in outs else t.share(t.slope.at[0], owner(y, xx, 1 - core))
        net.start(src, t.r.at[y, xx], partner, "swap" + "amby"[(ma, mb, my).index(t)], tag)
        if tag == "y2":
            net.start(sn, sn_other, partner, "sn", "sn")
            signal(hop_sem.at[0], up, down)
    for i, t in enumerate((ma, my, mb)):
        loaded(t.s, 2 + i)

    taken = [0]

    def take(tag):
        end = max(i for i, entry in enumerate(order) if entry[0] == tag) + 1
        for i in range(taken[0], end):
            name, t, y, xx = order[i]
            group = [j for j, entry in enumerate(order) if entry[0] == name]
            if i == group[0]:
                net.here(name, t.s.at[0, pl.ds(0, len(group))])
            add(t.s.at[y, xx], t.r.at[y, xx])
        taken[0] = max(taken[0], end)

    def x_send(t, h, xx, slot, target, stage):
        net.start(t.item(yh, h, xx), t.x_in.at[slot], target, t.name + "x", t.name + stage)

    def far(t):
        x_send(t, 0, x2, 0, right, "far")
        x_send(t, 1, x2, 1, left, "far")

    def near(t):
        x_send(t, 0, xl, 2, left, "near")
        x_send(t, 1, xr, 3, right, "near")

    def relay(t):
        net.here(t.name + "far", t.x_in.at[pl.ds(0, 2)])
        add(t.item(yh, 0, xr), t.x_in.at[0])
        x_send(t, 0, xr, 4, right, "near")
        add(t.item(yh, 1, xl), t.x_in.at[1])
        x_send(t, 1, xl, 5, left, "near")

    def settle(t):
        net.here(t.name + "near", t.x_in.at[pl.ds(2, 4)])
        for h in (0, 1):
            add(t.item(yh, h, x), t.x_in.at[2 + h], t.x_in.at[4 + h])

    def finish(t, extra=()):
        own = t.sums(yh, x)
        value = own[...]
        for e in extra:
            value = value + e[...]
        value = value * (replicas**-0.5)
        own[...] = value
        t.src[0:1, :] = t.squares(value)
        for k, peer in enumerate(others, 1):
            net.start(t.src, t.nm.at[k], peer, t.name + "norm", t.name + "norm")

    def update(t):
        total = t.src[...]
        net.here(t.name + "norm", t.nm.at[pl.ds(1, models - 1)])
        for k in range(1, models):
            total = total + t.nm[k]
        ratio = jnp.sqrt(total[1:2]) * lax.rsqrt(total[0:1] + EPS)
        if t.by_rows:
            ratio = jnp.broadcast_to(ratio, (ROWS, ROWS)).T[: t.rows]
            ratio = jnp.concatenate([ratio] * (t.p.shape[1] // ROWS), axis=1)
        new = t.p[...] - LEARN_RATE * (t.sums(yh, x)[...] * ratio)
        t.new[...] = new
        t.block(owner(yh, x, core))[...] = new.astype(jnp.bfloat16)

    def spread(t, y, xx, target, got):
        block = t.block(owner(y, xx, core))
        net.start(block, block, target, t.name + "half", t.name + got)

    def hand(t, y, xx):
        block = t.block(owner(y, xx, core))
        net.start(block, block, partner, t.name + "hand", t.name + "hand")

    def around(t, y, got):
        spread(t, y, x, right, got)
        spread(t, y, x, left, got)
        if t.direct:
            spread(t, y, x, beyond, got + "2")

    def wait(t, got, count):
        net.here(t.name + got, t.blocks(count))

    def rise(t):
        net.start(t.sums(yo, x), t.y, across, t.name + "y", t.name + "y")

    def risen(t):
        net.here(t.name + "y", t.y)
        finish(t, (t.y,))

    def y_send(xx, j):
        net.start(my.s.at[yo, xx], y_in.at[j], across, "y", "in%d" % j)

    def fold(xx, j):
        net.here("in%d" % j, y_in.at[j])
        add(my.s.at[yh, xx], y_in.at[j])

    def publish(t):
        update(t)
        spread(t, yh, x, across, "up")
        hand(t, yh, x)

    def second(t):
        wait(t, "up", 1)
        around(t, yo, "oth")
        hand(t, yo, x)

    def pass_own(t):
        wait(t, "own", 2)
        if not t.direct:
            spread(t, yh, xl, right, "own2")
        hand(t, yh, xl)
        hand(t, yh, xr)

    def pass_oth(t):
        wait(t, "oth", 2)
        if not t.direct:
            spread(t, yo, xr, left, "oth2")
        hand(t, yo, xl)
        hand(t, yo, xr)

    def last(t, y, got):
        wait(t, got, 1)
        hand(t, y, x2)

    def publish_y(t):
        update(t)
        around(t, yh, "own")
        spread(t, yh, x, across, "up0")
        hand(t, yh, x)

    def climb(t):
        wait(t, "own", 2)
        spread(t, yh, xl, across, "up1")
        spread(t, yh, xr, across, "up1")
        hand(t, yh, xl)
        hand(t, yh, xr)

    def climb2(t):
        wait(t, "own2", 1)
        spread(t, yh, x2, across, "up2")
        hand(t, yh, x2)

    def tell(y, target, got):
        row = gain.at[core, y * XS + x]
        net.start(row, row, target, "tell", got)

    def told(got, count):
        net.here(got, gain.at[0, pl.ds(0, count)])

    take("af")
    far(a1)
    far(a2)
    take("y0")
    y_send(x2, 0)
    take("an")
    near(a1)
    near(a2)
    take("y1")
    y_send(xr, 1)
    take("ar")
    take("y2")
    y_send(xl, 2)
    for i, t in enumerate((ma, mb, my)):
        loaded(t.p, 5 + i)
    for t in (ta, b1, b2, y1, y2):
        t.src[1:2, :] = t.squares(t.p[...])
    take("bf")
    relay(a1)
    take("yx2")
    relay(a2)
    loaded(sn_here, 9)
    net.here("sn", sn_other)
    for y in (0, 1):
        for xx in range(XS):
            at = pl.ds(pl.multiple_of(owner(y, xx, core) * ROWS, ROWS), ROWS)
            tn.s[y, xx] = sn_here[0:1, at] + sn_other[0:1, at]
    far(tn)
    near(tn)
    far(b1)
    far(b2)
    pl.semaphore_wait(hop_sem.at[0], 2)
    signal(hop_sem.at[1], up, down)
    take("bn")
    near(b1)
    fold(x2, 0)
    pl.semaphore_wait(hop_sem.at[1], 2)
    signal(hop_sem.at[2], up, down)
    take("yo")
    pl.semaphore_wait(hop_sem.at[2], 2)
    signal(hop_sem.at[3], beside)
    fold(xr, 1)
    net.gone("sn", sn_other)
    for name, t in (("swapa", ma), ("swapm", mb), ("swapb", my)):
        net.gone(name, t.s)
    settle(a1)
    rise(a1)
    settle(a2)
    rise(a2)
    y_send(x, 3)
    relay(tn)
    fold(xl, 2)
    relay(b1)
    near(b2)
    relay(b2)
    far(y1)
    far(y2)
    near(y1)
    near(y2)
    pl.semaphore_wait(hop_sem.at[3], 1)
    for t in (a1, a2):
        net.gone(t.name + "x", t.x_in)
        net.here(t.name + "y", t.y)
        add(t.sums(yh, x), t.y)
    finish(ta)
    settle(b1)
    rise(b1)
    fold(x, 3)
    publish(ta)
    settle(b2)
    rise(b2)
    relay(y1)
    risen(b1)
    relay(y2)
    around(ta, yh, "own")
    settle(tn)
    net.start(tn.s.at[yo, x], tn.y, across, "ny", "ny")
    second(ta)
    risen(b2)
    settle(y1)
    finish(y1)
    settle(y2)
    finish(y2)
    publish(b1)
    around(b1, yh, "own")
    loaded(pn_here, 8)
    net.here("ny", tn.y)
    add(tn.s.at[yh, x], tn.y)
    gain[core, yh * XS + x] = pn_here[...] - LEARN_RATE * (tn.s[yh, x] * (replicas**-0.5))
    nn[...] = gain[core, yh * XS + x]
    tell(yh, across, "nup")
    for target, got in ((right, "nown"), (left, "nown"), (beyond, "nown2")):
        tell(yh, target, got)
    pass_own(ta)
    for t in (a1, a2, b1, b2):
        net.gone(t.name + "y", t.y)
    net.gone("ny", tn.y)
    net.gone("y", y_in)
    net.gone("nx", tn.x_in)
    publish(b2)
    publish_y(y1)
    publish_y(y2)
    around(b2, yh, "own")
    pass_oth(ta)
    second(b1)
    pass_own(b1)
    told("nup", 1)
    for target, got in ((right, "noth"), (left, "noth"), (beyond, "noth2")):
        tell(yo, target, got)
    for t in (ta, b1, b2, y1, y2):
        net.gone(t.name + "norm", t.nm.at[pl.ds(1, models - 1)])
        if t is not ta:
            net.gone(t.name + "x", t.x_in)
    climb(y1)
    second(b2)
    climb2(y1)
    climb(y2)
    climb2(y2)
    pass_own(b2)
    pass_oth(b1)
    last(ta, yh, "own2")
    last(ta, yo, "oth2")
    told("nown", 2)
    told("nown2", 1)
    told("noth", 2)
    told("noth2", 1)
    net.start(gain.at[core], gain.at[core], partner, "nhand", "nhand")
    pass_oth(b2)
    for t in (y1, y2):
        wait(t, "up0", 1)
        hand(t, yo, x)
    net.here("nhand", gain.at[core])
    for y in (0, 1):
        for xx in range(XS):
            for c in (0, 1):
                at = owner(y, xx, c) * ROWS
                hn[at : at + ROWS] = gain[c, y * XS + xx, 0, :].astype(jnp.bfloat16)
    net.gone("nhand", gain.at[core])
    net.gone("tell", gain.at[0, pl.ds(0, 7)])
    net.gone("ahalf", ta.blocks(7))
    last(b1, yh, "own2")
    net.here("ahand", ta.blocks(8))
    net.gone("ahand", ta.blocks(8))

    def top(t):
        wait(t, "up1", 2)
        hand(t, yo, xl)
        hand(t, yo, xr)

    top(y1)
    last(b1, yo, "oth2")
    last(b2, yh, "own2")
    top(y2)
    last(y1, yo, "up2")
    last(b2, yo, "oth2")
    last(y2, yo, "up2")
    for t in (b1, y1, b2, y2):
        net.here(t.name + "hand", t.blocks(8))
        net.gone(t.name + "half", t.blocks(7))
        net.gone(t.name + "hand", t.blocks(8))


def store(*refs):
    copies = [
        pltpu.make_async_copy(refs[i], refs[8 + i], refs[16].at[i]) for i in range(8)
    ]
    for copy in copies:
        copy.start()
    for copy in copies:
        copy.wait()


def body(sg, su, sd, sn, pg, pu, pd, pn):
    arrays = (sg, su, sd, sn, pg, pu, pd, pn.reshape(1, ROWS))
    replicas, models = lax.axis_size("replica"), lax.axis_size("model")
    width, cols = sg.shape[1:]
    f32, bf16 = jnp.float32, jnp.bfloat16

    def matrix(share):
        sums = pltpu.VMEM((2, XS, *share), f32)
        return [sums, sums, pltpu.VMEM(share, f32)]

    def scratch(block, x_first):
        item = block if x_first else (block[0] // 2, block[1])
        arrived = [pltpu.VMEM((6, *item), f32)] + [pltpu.VMEM(block, f32)] * x_first
        return arrived + [pltpu.VMEM((2, ROWS), f32), pltpu.VMEM((models, 2, ROWS), f32)]

    vmem = pl.BlockSpec(memory_space=pltpu.VMEM)
    hbm = pl.BlockSpec(memory_space=pltpu.HBM)
    shape = jax.ShapeDtypeStruct
    out = pl.pallas_call(
        functools.partial(kernel, replicas, models),
        out_shape=(
            shape((width, cols), bf16),
            shape((width, cols), bf16),
            shape((cols, width), bf16),
            shape((width,), bf16),
            shape((ROWS, cols), f32),
            shape((ROWS, cols), f32),
            shape((cols, ROWS), f32),
            shape((1, ROWS), f32),
        ),
        in_specs=[hbm] * 8,
        out_specs=(vmem,) * 8,
        scratch_shapes=[
            *matrix((ROWS, cols)),
            *matrix((ROWS, cols)),
            *matrix((cols, ROWS)),
            *scratch((cols // 2, ROWS), True),
            *scratch((cols // 2, ROWS), True)[:2],
            *scratch((ROWS // 2, cols), True),
            *scratch((ROWS // 2, cols), True),
            *scratch((ROWS // 2, cols), False),
            *scratch((ROWS // 2, cols), False),
            pltpu.VMEM((XS, ROWS, cols), f32),
            pltpu.VMEM((2, XS, 1, ROWS), f32),
            pltpu.VMEM((6, 1, ROWS), f32),
            pltpu.VMEM((1, ROWS), f32),
            pltpu.VMEM((2, 2 * XS, 1, ROWS), f32),
            pltpu.VMEM((1, ROWS), f32),
            pltpu.VMEM((1, width), f32),
            pltpu.VMEM((1, width), f32),
            pltpu.VMEM((4, cols, ROWS), f32),
            pltpu.VMEM((1, ROWS, cols), f32),
            pltpu.SemaphoreType.DMA((10,)),
            pltpu.SemaphoreType.DMA((SENDS,)),
            pltpu.SemaphoreType.DMA((RECVS,)),
            pltpu.SemaphoreType.REGULAR((4,)),
        ],
        compiler_params=pltpu.CompilerParams(
            collective_id=0, has_side_effects=True, vmem_limit_bytes=32 << 20
        ),
    )(*(pltpu.with_memory_space_constraint(a, pltpu.HBM) for a in arrays))
    out = (*out[:3], out[3].reshape(width), *out[4:])
    out = pl.pallas_call(
        store,
        out_shape=tuple(shape(o.shape, o.dtype) for o in out),
        in_specs=[vmem] * 8,
        out_specs=(hbm,) * 8,
        scratch_shapes=[pltpu.SemaphoreType.DMA((8,))],
        compiler_params=pltpu.CompilerParams(vmem_limit_bytes=8 << 20),
    )(*(pltpu.with_memory_space_constraint(o, pltpu.VMEM) for o in out))
    return (*out[:7], out[7].reshape(ROWS))


def solution(mesh):
    return jax.shard_map(
        body,
        mesh=mesh,
        in_specs=(
            P("replica", None, "model"),
            P("replica", None, "model"),
            P("replica", "model", None),
            P("replica", None),
            P("replica", "model"),
            P("replica", "model"),
            P("model", "replica"),
            P("replica"),
        ),
        out_specs=(
            P(None, "model"),
            P(None, "model"),
            P("model", None),
            P(),
            P("replica", "model"),
            P("replica", "model"),
            P("model", "replica"),
            P("replica"),
        ),
        check_vma=False,
    )
```

```python
import functools

import jax
import jax.numpy as jnp
from jax import lax
from jax.experimental import pallas as pl
from jax.experimental.pallas import tpu as pltpu
from jax.sharding import PartitionSpec as P

MESH = pl.DeviceIdType.MESH
LEARN_RATE = 0.5
EPS = 1e-06
ROWS = 128
XS = 4
TURNED = 16
SENDS, RECVS = 36, 86


class Copies:
    def __init__(self, send, recv):
        self.send, self.recv, self.sends, self.recvs = send, recv, {}, {}

    def start(self, src, dst, target, sent, got):
        pltpu.make_async_remote_copy(
            src_ref=src,
            dst_ref=dst,
            send_sem=self.send.at[self.sends.setdefault(sent, len(self.sends))],
            recv_sem=self.recv.at[self.recvs.setdefault(got, len(self.recvs))],
            device_id=target,
            device_id_type=MESH,
        ).start()

    def gone(self, sent, size):
        pltpu.make_async_copy(size, size, self.send.at[self.sends[sent]]).wait()

    def here(self, got, size):
        pltpu.make_async_copy(size, size, self.recv.at[self.recvs[got]]).wait()


class Matrix:
    def __init__(self, by_rows, slope, param, half, new, s, r, p):
        self.by_rows, self.slope, self.param, self.half, self.new = by_rows, slope, param, half, new
        self.s, self.r, self.p = s, r, p

    def share(self, ref, index):
        at = pl.ds(pl.multiple_of(index * ROWS, ROWS), ROWS)
        return ref.at[at, :] if self.by_rows else ref.at[:, at]


class Tensor:
    def __init__(self, name, whole, x_first, direct, low, rows, x_in, y, src, nm):
        self.name, self.whole, self.x_first, self.direct = name, whole, x_first, direct
        self.low, self.rows, self.x_in, self.y, self.src, self.nm = low, rows, x_in, y, src, nm
        self.by_rows = whole.by_rows
        self.p = whole.p.at[pl.ds(low, rows)]
        self.new = whole.new.at[pl.ds(low, rows)]

    def blocks(self, count):
        if self.by_rows:
            return self.whole.half.at[pl.ds(0, count * self.rows), :]
        return self.whole.half.at[:, pl.ds(0, count * ROWS)]

    def sums(self, y, x):
        return self.whole.s.at[y, x, pl.ds(self.low, self.rows)]

    def block(self, index):
        return self.part(index, 0, self.rows)

    def part(self, index, at, rows):
        at = self.low + at
        if self.by_rows:
            at = pl.ds(pl.multiple_of(index * ROWS + at, rows), rows)
            return self.whole.half.at[at, :]
        return self.whole.half.at[pl.ds(at, rows), pl.ds(pl.multiple_of(index * ROWS, ROWS), ROWS)]

    def item(self, yh, h, x):
        if self.x_first:
            return self.sums(h, x)
        size = self.rows // 2
        return self.whole.s.at[yh, x, pl.ds(self.low + h * size, size)]

    def squares(self, value):
        value = value * value
        if not self.by_rows:
            return jnp.sum(value, axis=0, keepdims=True)
        folded = value[:, :ROWS]
        for at in range(ROWS, value.shape[1], ROWS):
            folded = folded + value[:, at : at + ROWS]
        if self.rows < ROWS:
            folded = jnp.concatenate([folded, jnp.zeros_like(folded)], axis=0)
        return jnp.sum(folded.T, axis=0, keepdims=True)


class Vector:
    name, x_first = "n", True

    def __init__(self, s, x_in, y):
        self.s, self.x_in, self.y = s, x_in, y

    def item(self, yh, h, x):
        return self.s.at[h, x]


def add(into, *others):
    value = into[...]
    for other in others:
        value = value + other[...]
    into[...] = value


def kernel(replicas, models, *refs):
    (sg, su, sd, sn, pg, pu, pd, pn), refs = refs[:8], refs[8:]
    (hg, hu, hd, hn, ng, nu, nd, nn), refs = refs[:8], refs[8:]
    my, refs = Matrix(True, sg, pg, hg, ng, *refs[:3]), refs[3:]
    mb, refs = Matrix(True, su, pu, hu, nu, *refs[:3]), refs[3:]
    ma, refs = Matrix(False, sd, pd, hd, nd, *refs[:3]), refs[3:]
    half = ROWS // 2
    deep = ma.p.shape[0]
    ta = Tensor("a", ma, True, False, 0, deep, None, None, *refs[2:4])
    a1 = Tensor("a1", ma, True, False, 0, deep // 2, *refs[:2], None, None)
    refs = refs[4:]
    a2 = Tensor("a2", ma, True, False, deep // 2, deep // 2, *refs[:2], None, None)
    refs = refs[2:]
    b1, refs = Tensor("b1", mb, True, False, 0, half, *refs[:4]), refs[4:]
    straight = half - TURNED
    b2 = Tensor("b2", mb, True, False, half, half, None, None, *refs[2:4])
    b3 = Tensor("b3", mb, True, False, half, straight, *refs[:2], None, None)
    refs = refs[4:]
    b4 = Tensor("b4", mb, False, False, half + straight, TURNED, refs[0], None, None, None)
    b4_in, refs = refs[1], refs[2:]
    y1, refs = Tensor("y1", my, False, True, 0, half, refs[0], None, *refs[1:3]), refs[3:]
    y2, refs = Tensor("y2", my, False, True, half, half, refs[0], None, *refs[1:3]), refs[3:]
    y_in, refs = refs[0], refs[1:]
    tn, refs = Vector(*refs[:3]), refs[3:]
    gain, pn_here, sn_here, sn_other, a_out, y_out, refs = *refs[:6], refs[6:]
    local_sem, send_sem, recv_sem, hop_sem = refs

    r = lax.axis_index("replica")
    m = lax.axis_index("model")
    core = r % 2
    x = (r // 2) % XS
    yh = r // (2 * XS)
    yo = 1 - yh
    xr, xl, x2 = (x + 1) % XS, (x + XS - 1) % XS, (x + 2) % XS

    def owner(y, xx, c):
        return (y * XS + xx) * 2 + c

    def device(y, xx, c):
        return {"replica": owner(y, xx, c), "model": m}

    right, left = device(yh, xr, core), device(yh, xl, core)
    across, partner = device(yo, x, core), device(yh, x, 1 - core)
    beyond = device(yh, x2, core)
    net = Copies(send_sem, recv_sem)
    others = [{"replica": r, "model": (m + k) % models} for k in range(1, models)]
    zs = models // 2
    z, yl = m // 2, m % 2
    up = {"replica": r, "model": (z + 1) % zs * 2 + yl}
    down = {"replica": r, "model": (z + zs - 1) % zs * 2 + yl}
    beside = {"replica": r, "model": z * 2 + 1 - yl}

    def signal(sem, *peers):
        for peer in peers:
            pl.semaphore_signal(sem, inc=1, device_id=peer, device_id_type=MESH)

    barrier = pltpu.get_barrier_semaphore()
    signal(barrier, partner, right, left, across, up, down, beside)

    order = [("af", ma, 0, x2), ("af", ma, 1, x2), ("y0", my, yo, x2)]
    order += [("an", ma, 1, xr), ("an", ma, 0, xl), ("y1", my, yo, xr)]
    order += [("ar", ma, 0, xr), ("ar", ma, 1, xl), ("y2", my, yo, xl)]
    order += [("bf", mb, 0, x2), ("bf", mb, 1, x2), ("y3", my, yo, x)]
    order += [("yx2", my, yh, x2), ("bn", mb, 1, xr), ("bn", mb, 0, xl)]
    order += [("br", mb, 0, xr), ("br", mb, 1, xl), ("yx", my, yh, xr)]
    order += [("yx", my, yh, xl), ("ao", ma, 0, x), ("ao", ma, 1, x)]
    order += [("bo", mb, 0, x), ("bo", mb, 1, x), ("yo", my, yh, x)]
    def load(src, dst, sem):
        pltpu.make_async_copy(src, dst, local_sem.at[sem]).start()

    def loaded(ref, sem):
        pltpu.make_async_copy(ref, ref, local_sem.at[sem]).wait()

    early, outs = {"af": ma, "an": ma, "y0": my}, {}
    for i, (tag, t, y, xx) in enumerate(order):
        if tag in early:
            n = len([k for k in outs if order[k][1] is t])
            outs[i] = (a_out if t is ma else y_out).at[n]
            load(t.share(t.slope.at[0], owner(y, xx, 1 - core)), outs[i], 0 if t is ma else 1)
    for tag, t, y, xx in order:
        load(t.share(t.slope.at[0], owner(y, xx, core)), t.s.at[y, xx], (ma, my, mb).index(t) + 2)
    for i, t in enumerate((ma, mb, my)):
        load(t.param, t.p, 5 + i)
    load(pn, pn_here, 8)
    load(sn, sn_here, 9)
    loaded(a_out, 0)
    loaded(y_out, 1)
    pl.semaphore_wait(barrier, 7)

    for i, (tag, t, y, xx) in enumerate(order):
        src = outs[i] if i in outs else t.share(t.slope.at[0], owner(y, xx, 1 - core))
        net.start(src, t.r.at[y, xx], partner, "swap" + "amby"[(ma, mb, my).index(t)], tag)
        if tag == "y2":
            net.start(sn, sn_other, partner, "sn", "sn")
            signal(hop_sem.at[0], up, down)
    for i, t in enumerate((ma, my, mb)):
        loaded(t.s, 2 + i)

    taken = [0]

    def take(tag):
        end = max(i for i, entry in enumerate(order) if entry[0] == tag) + 1
        for i in range(taken[0], end):
            name, t, y, xx = order[i]
            group = [j for j, entry in enumerate(order) if entry[0] == name]
            if i == group[0]:
                net.here(name, t.s.at[0, pl.ds(0, len(group))])
            add(t.s.at[y, xx], t.r.at[y, xx])
        taken[0] = max(taken[0], end)

    def x_send(t, h, xx, slot, target, stage):
        net.start(t.item(yh, h, xx), t.x_in.at[slot], target, t.name + "x", t.name + stage)

    def far(t):
        x_send(t, 0, x2, 0, right, "far")
        x_send(t, 1, x2, 1, left, "far")

    def near(t):
        x_send(t, 0, xl, 2, left, "near")
        x_send(t, 1, xr, 3, right, "near")

    def relay(t):
        net.here(t.name + "far", t.x_in.at[pl.ds(0, 2)])
        add(t.item(yh, 0, xr), t.x_in.at[0])
        x_send(t, 0, xr, 4, right, "near")
        add(t.item(yh, 1, xl), t.x_in.at[1])
        x_send(t, 1, xl, 5, left, "near")

    def settle(t):
        net.here(t.name + "near", t.x_in.at[pl.ds(2, 4)])
        for h in (0, 1):
            add(t.item(yh, h, x), t.x_in.at[2 + h], t.x_in.at[4 + h])

    def finish(t, extra=()):
        own = t.sums(yh, x)
        value = own[...]
        for e in extra:
            value = value + e[...]
        value = value * (replicas**-0.5)
        own[...] = value
        t.src[0:1, :] = t.squares(value)
        for k, peer in enumerate(others, 1):
            net.start(t.src, t.nm.at[k], peer, t.name + "norm", t.name + "norm")

    def update(t):
        total = t.src[...]
        net.here(t.name + "norm", t.nm.at[pl.ds(1, models - 1)])
        for k in range(1, models):
            total = total + t.nm[k]
        ratio = jnp.sqrt(total[1:2]) * lax.rsqrt(total[0:1] + EPS)
        if t.by_rows:
            ratio = jnp.broadcast_to(ratio, (ROWS, ROWS)).T[: t.rows]
            ratio = jnp.concatenate([ratio] * (t.p.shape[1] // ROWS), axis=1)
        new = t.p[...] - LEARN_RATE * (t.sums(yh, x)[...] * ratio)
        t.new[...] = new
        t.block(owner(yh, x, core))[...] = new.astype(jnp.bfloat16)

    def spread(t, y, xx, target, got):
        block = t.block(owner(y, xx, core))
        net.start(block, block, target, t.name + "half", t.name + got)

    def hand(t, y, xx):
        block = t.block(owner(y, xx, core))
        net.start(block, block, partner, t.name + "hand", t.name + "hand")

    def around(t, y, got):
        spread(t, y, x, right, got)
        spread(t, y, x, left, got)
        if t.direct:
            spread(t, y, x, beyond, got + "2")

    def wait(t, got, count):
        net.here(t.name + got, t.blocks(count))

    def rise(t):
        net.start(t.sums(yo, x), t.y, across, t.name + "y", t.name + "y")

    def risen(t):
        net.here(t.name + "y", t.y)
        finish(t, (t.y,))

    def y_send(xx, j):
        net.start(my.s.at[yo, xx], y_in.at[j], across, "y", "in%d" % j)

    def fold(xx, j):
        net.here("in%d" % j, y_in.at[j])
        add(my.s.at[yh, xx], y_in.at[j])

    def turn(xx, j):
        net.start(b4.sums(yo, xx), b4_in.at[j], across, "b4y", "b4in%d" % j)

    def turned(xx, j):
        net.here("b4in%d" % j, b4_in.at[j])
        add(b4.sums(yh, xx), b4_in.at[j])

    def publish(t):
        update(t)
        spread(t, yh, x, across, "up")
        hand(t, yh, x)

    def second(t):
        wait(t, "up", 1)
        around(t, yo, "oth")
        hand(t, yo, x)

    def pass_own(t):
        wait(t, "own", 2)
        if not t.direct:
            spread(t, yh, xl, right, "own2")
        hand(t, yh, xl)
        hand(t, yh, xr)

    def pass_oth(t):
        wait(t, "oth", 2)
        if not t.direct:
            spread(t, yo, xr, left, "oth2")
        hand(t, yo, xl)
        hand(t, yo, xr)

    def last(t, y, got):
        wait(t, got, 1)
        hand(t, y, x2)

    def publish_y(t):
        update(t)
        around(t, yh, "own")
        spread(t, yh, x, across, "up0")
        hand(t, yh, x)

    def climb(t):
        wait(t, "own", 2)
        spread(t, yh, xl, across, "up1")
        spread(t, yh, xr, across, "up1")
        hand(t, yh, xl)
        hand(t, yh, xr)

    def climb2(t):
        wait(t, "own2", 1)
        spread(t, yh, x2, across, "up2")
        hand(t, yh, x2)

    def tell(y, target, got):
        row = gain.at[core, y * XS + x]
        net.start(row, row, target, "tell", got)

    def told(got, count):
        net.here(got, gain.at[0, pl.ds(0, count)])

    take("af")
    far(a1)
    far(a2)
    take("y0")
    y_send(x2, 0)
    take("an")
    near(a1)
    near(a2)
    take("y1")
    y_send(xr, 1)
    take("ar")
    take("y2")
    y_send(xl, 2)
    for i, t in enumerate((ma, mb, my)):
        loaded(t.p, 5 + i)
    for t in (ta, b1, b2, y1, y2):
        t.src[1:2, :] = t.squares(t.p[...])
    take("bf")
    relay(a1)
    take("yx2")
    relay(a2)
    loaded(sn_here, 9)
    net.here("sn", sn_other)
    for y in (0, 1):
        for xx in range(XS):
            at = pl.ds(pl.multiple_of(owner(y, xx, core) * ROWS, ROWS), ROWS)
            tn.s[y, xx] = sn_here[0:1, at] + sn_other[0:1, at]
    far(tn)
    near(tn)
    far(b1)
    far(b3)
    pl.semaphore_wait(hop_sem.at[0], 2)
    signal(hop_sem.at[1], up, down)
    take("bn")
    near(b1)
    fold(x2, 0)
    pl.semaphore_wait(hop_sem.at[1], 2)
    signal(hop_sem.at[2], up, down)
    take("yo")
    pl.semaphore_wait(hop_sem.at[2], 2)
    signal(hop_sem.at[3], beside)
    turn(x2, 0)
    turn(xr, 1)
    turn(xl, 2)
    fold(xr, 1)
    net.gone("sn", sn_other)
    for name, t in (("swapa", ma), ("swapm", mb), ("swapb", my)):
        net.gone(name, t.s)
    settle(a1)
    rise(a1)
    settle(a2)
    rise(a2)
    y_send(x, 3)
    turn(x, 3)
    relay(tn)
    fold(xl, 2)
    relay(b1)
    near(b3)
    turned(x2, 0)
    far(b4)
    relay(b3)
    turned(xr, 1)
    turned(xl, 2)
    near(b4)
    far(y1)
    far(y2)
    near(y1)
    near(y2)
    pl.semaphore_wait(hop_sem.at[3], 1)
    for t in (a1, a2):
        net.gone(t.name + "x", t.x_in)
        net.here(t.name + "y", t.y)
        add(t.sums(yh, x), t.y)
    finish(ta)
    settle(b1)
    rise(b1)
    publish(ta)
    settle(b3)
    rise(b3)
    relay(b4)
    relay(y1)
    risen(b1)
    relay(y2)
    around(ta, yh, "own")
    settle(tn)
    net.start(tn.s.at[yo, x], tn.y, across, "ny", "ny")
    fold(x, 3)
    turned(x, 3)
    settle(b4)
    net.here("b3y", b3.y)
    add(b3.sums(yh, x), b3.y)
    finish(b2)
    settle(y1)
    finish(y1)
    settle(y2)
    finish(y2)
    second(ta)
    publish(b1)
    around(b1, yh, "own")
    loaded(pn_here, 8)
    net.here("ny", tn.y)
    add(tn.s.at[yh, x], tn.y)
    gain[core, yh * XS + x] = pn_here[...] - LEARN_RATE * (tn.s[yh, x] * (replicas**-0.5))
    nn[...] = gain[core, yh * XS + x]
    tell(yh, across, "nup")
    for target, got in ((right, "nown"), (left, "nown"), (beyond, "nown2")):
        tell(yh, target, got)
    pass_own(ta)
    for t in (a1, a2, b1, b3):
        net.gone(t.name + "y", t.y)
    net.gone("b4y", b4_in)
    net.gone("ny", tn.y)
    net.gone("y", y_in)
    net.gone("nx", tn.x_in)
    publish(b2)
    publish_y(y1)
    publish_y(y2)
    around(b2, yh, "own")
    pass_oth(ta)
    second(b1)
    pass_own(b1)
    told("nup", 1)
    for target, got in ((right, "noth"), (left, "noth"), (beyond, "noth2")):
        tell(yo, target, got)
    for t in (ta, b1, b2, y1, y2):
        net.gone(t.name + "norm", t.nm.at[pl.ds(1, models - 1)])
    for t in (b1, b3, b4, y1, y2):
        net.gone(t.name + "x", t.x_in)
    climb(y1)
    second(b2)
    climb2(y1)
    climb(y2)
    climb2(y2)
    pass_own(b2)
    pass_oth(b1)
    last(ta, yh, "own2")
    last(ta, yo, "oth2")
    told("nown", 2)
    told("nown2", 1)
    told("noth", 2)
    told("noth2", 1)
    net.start(gain.at[core], gain.at[core], partner, "nhand", "nhand")
    pass_oth(b2)
    for t in (y1, y2):
        wait(t, "up0", 1)
        hand(t, yo, x)
    net.here("nhand", gain.at[core])
    for y in (0, 1):
        for xx in range(XS):
            for c in (0, 1):
                at = owner(y, xx, c) * ROWS
                hn[at : at + ROWS] = gain[c, y * XS + xx, 0, :].astype(jnp.bfloat16)
    net.gone("nhand", gain.at[core])
    net.gone("tell", gain.at[0, pl.ds(0, 7)])
    net.gone("ahalf", ta.blocks(7))
    last(b1, yh, "own2")
    net.here("ahand", ta.blocks(8))
    net.gone("ahand", ta.blocks(8))

    def top(t):
        wait(t, "up1", 2)
        hand(t, yo, xl)
        hand(t, yo, xr)

    top(y1)
    last(b1, yo, "oth2")
    last(b2, yh, "own2")
    top(y2)
    last(y1, yo, "up2")
    last(b2, yo, "oth2")
    last(y2, yo, "up2")
    for t in (b1, y1, b2, y2):
        net.here(t.name + "hand", t.blocks(8))
        net.gone(t.name + "half", t.blocks(7))
        net.gone(t.name + "hand", t.blocks(8))


def store(*refs):
    copies = [
        pltpu.make_async_copy(refs[i], refs[8 + i], refs[16].at[i]) for i in range(8)
    ]
    for copy in copies:
        copy.start()
    for copy in copies:
        copy.wait()


def body(sg, su, sd, sn, pg, pu, pd, pn):
    arrays = (sg, su, sd, sn, pg, pu, pd, pn.reshape(1, ROWS))
    replicas, models = lax.axis_size("replica"), lax.axis_size("model")
    width, cols = sg.shape[1:]
    f32, bf16 = jnp.float32, jnp.bfloat16

    def matrix(share):
        sums = pltpu.VMEM((2, XS, *share), f32)
        return [sums, sums, pltpu.VMEM(share, f32)]

    def scratch(block, x_first):
        item = block if x_first else (block[0] // 2, block[1])
        arrived = [pltpu.VMEM((6, *item), f32)] + [pltpu.VMEM(block, f32)] * x_first
        return arrived + [pltpu.VMEM((2, ROWS), f32), pltpu.VMEM((models, 2, ROWS), f32)]

    vmem = pl.BlockSpec(memory_space=pltpu.VMEM)
    hbm = pl.BlockSpec(memory_space=pltpu.HBM)
    shape = jax.ShapeDtypeStruct
    out = pl.pallas_call(
        functools.partial(kernel, replicas, models),
        out_shape=(
            shape((width, cols), bf16),
            shape((width, cols), bf16),
            shape((cols, width), bf16),
            shape((width,), bf16),
            shape((ROWS, cols), f32),
            shape((ROWS, cols), f32),
            shape((cols, ROWS), f32),
            shape((1, ROWS), f32),
        ),
        in_specs=[hbm] * 8,
        out_specs=(vmem,) * 8,
        scratch_shapes=[
            *matrix((ROWS, cols)),
            *matrix((ROWS, cols)),
            *matrix((cols, ROWS)),
            *scratch((cols // 2, ROWS), True),
            *scratch((cols // 2, ROWS), True)[:2],
            *scratch((ROWS // 2, cols), True),
            *scratch((ROWS // 2 - TURNED, cols), True),
            pltpu.VMEM((6, TURNED // 2, cols), f32),
            pltpu.VMEM((XS, TURNED, cols), f32),
            *scratch((ROWS // 2, cols), False),
            *scratch((ROWS // 2, cols), False),
            pltpu.VMEM((XS, ROWS, cols), f32),
            pltpu.VMEM((2, XS, 1, ROWS), f32),
            pltpu.VMEM((6, 1, ROWS), f32),
            pltpu.VMEM((1, ROWS), f32),
            pltpu.VMEM((2, 2 * XS, 1, ROWS), f32),
            pltpu.VMEM((1, ROWS), f32),
            pltpu.VMEM((1, width), f32),
            pltpu.VMEM((1, width), f32),
            pltpu.VMEM((4, cols, ROWS), f32),
            pltpu.VMEM((1, ROWS, cols), f32),
            pltpu.SemaphoreType.DMA((10,)),
            pltpu.SemaphoreType.DMA((SENDS,)),
            pltpu.SemaphoreType.DMA((RECVS,)),
            pltpu.SemaphoreType.REGULAR((4,)),
        ],
        compiler_params=pltpu.CompilerParams(
            collective_id=0, has_side_effects=True, vmem_limit_bytes=32 << 20
        ),
    )(*(pltpu.with_memory_space_constraint(a, pltpu.HBM) for a in arrays))
    out = (*out[:3], out[3].reshape(width), *out[4:])
    out = pl.pallas_call(
        store,
        out_shape=tuple(shape(o.shape, o.dtype) for o in out),
        in_specs=[vmem] * 8,
        out_specs=(hbm,) * 8,
        scratch_shapes=[pltpu.SemaphoreType.DMA((8,))],
        compiler_params=pltpu.CompilerParams(vmem_limit_bytes=8 << 20),
    )(*(pltpu.with_memory_space_constraint(o, pltpu.VMEM) for o in out))
    return (*out[:7], out[7].reshape(ROWS))


def solution(mesh):
    return jax.shard_map(
        body,
        mesh=mesh,
        in_specs=(
            P("replica", None, "model"),
            P("replica", None, "model"),
            P("replica", "model", None),
            P("replica", None),
            P("replica", "model"),
            P("replica", "model"),
            P("model", "replica"),
            P("replica"),
        ),
        out_specs=(
            P(None, "model"),
            P(None, "model"),
            P("model", None),
            P(),
            P("replica", "model"),
            P("replica", "model"),
            P("model", "replica"),
            P("replica"),
        ),
        check_vma=False,
    )
```

```python
import functools

import jax
import jax.numpy as jnp
from jax import lax
from jax.experimental import pallas as pl
from jax.experimental.pallas import tpu as pltpu
from jax.sharding import PartitionSpec as P

MESH = pl.DeviceIdType.MESH
LEARN_RATE = 0.5
EPS = 1e-06
ROWS = 128
XS = 4
TURNED = 16
SENDS, RECVS = 36, 86


class Copies:
    def __init__(self, send, recv):
        self.send, self.recv, self.sends, self.recvs = send, recv, {}, {}

    def start(self, src, dst, target, sent, got):
        pltpu.make_async_remote_copy(
            src_ref=src,
            dst_ref=dst,
            send_sem=self.send.at[self.sends.setdefault(sent, len(self.sends))],
            recv_sem=self.recv.at[self.recvs.setdefault(got, len(self.recvs))],
            device_id=target,
            device_id_type=MESH,
        ).start()

    def gone(self, sent, size):
        pltpu.make_async_copy(size, size, self.send.at[self.sends[sent]]).wait()

    def here(self, got, size):
        pltpu.make_async_copy(size, size, self.recv.at[self.recvs[got]]).wait()


class Matrix:
    def __init__(self, by_rows, slope, param, half, new, s, r, p):
        self.by_rows, self.slope, self.param, self.half, self.new = by_rows, slope, param, half, new
        self.s, self.r, self.p = s, r, p

    def share(self, ref, index):
        at = pl.ds(pl.multiple_of(index * ROWS, ROWS), ROWS)
        return ref.at[at, :] if self.by_rows else ref.at[:, at]


class Tensor:
    def __init__(self, name, whole, x_first, direct, low, rows, x_in, y, src, nm):
        self.name, self.whole, self.x_first, self.direct = name, whole, x_first, direct
        self.low, self.rows, self.x_in, self.y, self.src, self.nm = low, rows, x_in, y, src, nm
        self.by_rows = whole.by_rows
        self.p = whole.p.at[pl.ds(low, rows)]
        self.new = whole.new.at[pl.ds(low, rows)]

    def blocks(self, count):
        if self.by_rows:
            return self.whole.half.at[pl.ds(0, count * self.rows), :]
        return self.whole.half.at[:, pl.ds(0, count * ROWS)]

    def sums(self, y, x):
        return self.whole.s.at[y, x, pl.ds(self.low, self.rows)]

    def block(self, index):
        return self.part(index, 0, self.rows)

    def part(self, index, at, rows):
        at = self.low + at
        if self.by_rows:
            at = pl.ds(pl.multiple_of(index * ROWS + at, rows), rows)
            return self.whole.half.at[at, :]
        return self.whole.half.at[pl.ds(at, rows), pl.ds(pl.multiple_of(index * ROWS, ROWS), ROWS)]

    def item(self, yh, h, x):
        if self.x_first:
            return self.sums(h, x)
        size = self.rows // 2
        return self.whole.s.at[yh, x, pl.ds(self.low + h * size, size)]

    def squares(self, value):
        value = value * value
        if not self.by_rows:
            return jnp.sum(value, axis=0, keepdims=True)
        folded = value[:, :ROWS]
        for at in range(ROWS, value.shape[1], ROWS):
            folded = folded + value[:, at : at + ROWS]
        if self.rows < ROWS:
            folded = jnp.concatenate([folded, jnp.zeros_like(folded)], axis=0)
        return jnp.sum(folded.T, axis=0, keepdims=True)


class Vector:
    name, x_first = "n", True

    def __init__(self, s, x_in, y):
        self.s, self.x_in, self.y = s, x_in, y

    def item(self, yh, h, x):
        return self.s.at[h, x]


def add(into, *others):
    value = into[...]
    for other in others:
        value = value + other[...]
    into[...] = value


def kernel(replicas, models, *refs):
    (sg, su, sd, sn, pg, pu, pd, pn), refs = refs[:8], refs[8:]
    (hg, hu, hd, hn, ng, nu, nd, nn), refs = refs[:8], refs[8:]
    my, refs = Matrix(True, sg, pg, hg, ng, *refs[:3]), refs[3:]
    mb, refs = Matrix(True, su, pu, hu, nu, *refs[:3]), refs[3:]
    ma, refs = Matrix(False, sd, pd, hd, nd, *refs[:3]), refs[3:]
    half = ROWS // 2
    deep = ma.p.shape[0]
    ta = Tensor("a", ma, True, False, 0, deep, None, None, *refs[2:4])
    a1 = Tensor("a1", ma, True, False, 0, deep // 2, *refs[:2], None, None)
    refs = refs[4:]
    a2 = Tensor("a2", ma, True, False, deep // 2, deep // 2, *refs[:2], None, None)
    refs = refs[2:]
    b1, refs = Tensor("b1", mb, True, False, 0, half, *refs[:4]), refs[4:]
    straight = half - TURNED
    b2 = Tensor("b2", mb, True, False, half, half, None, None, *refs[2:4])
    b3 = Tensor("b3", mb, True, False, half, straight, *refs[:2], None, None)
    refs = refs[4:]
    b4 = Tensor("b4", mb, False, False, half + straight, TURNED, refs[0], None, None, None)
    b4_in, refs = refs[1], refs[2:]
    y1, refs = Tensor("y1", my, False, True, 0, half, refs[0], None, *refs[1:3]), refs[3:]
    y2, refs = Tensor("y2", my, False, True, half, half, refs[0], None, *refs[1:3]), refs[3:]
    y_in, refs = refs[0], refs[1:]
    tn, refs = Vector(*refs[:3]), refs[3:]
    gain, pn_here, sn_here, sn_other, a_out, y_out, refs = *refs[:6], refs[6:]
    local_sem, send_sem, recv_sem, hop_sem = refs

    r = lax.axis_index("replica")
    m = lax.axis_index("model")
    core = r % 2
    x = (r // 2) % XS
    yh = r // (2 * XS)
    yo = 1 - yh
    xr, xl, x2 = (x + 1) % XS, (x + XS - 1) % XS, (x + 2) % XS

    def owner(y, xx, c):
        return (y * XS + xx) * 2 + c

    def device(y, xx, c):
        return {"replica": owner(y, xx, c), "model": m}

    right, left = device(yh, xr, core), device(yh, xl, core)
    across, partner = device(yo, x, core), device(yh, x, 1 - core)
    beyond = device(yh, x2, core)
    net = Copies(send_sem, recv_sem)
    others = [{"replica": r, "model": (m + k) % models} for k in range(1, models)]
    zs = models // 2
    z, yl = m // 2, m % 2
    up = {"replica": r, "model": (z + 1) % zs * 2 + yl}
    down = {"replica": r, "model": (z + zs - 1) % zs * 2 + yl}
    beside = {"replica": r, "model": z * 2 + 1 - yl}

    def signal(sem, *peers):
        for peer in peers:
            pl.semaphore_signal(sem, inc=1, device_id=peer, device_id_type=MESH)

    barrier = pltpu.get_barrier_semaphore()
    signal(barrier, partner, right, left, across, up, down, beside)

    order = [("af", ma, 0, x2), ("af", ma, 1, x2), ("y0", my, yo, x2)]
    order += [("an", ma, 1, xr), ("an", ma, 0, xl), ("y1", my, yo, xr)]
    order += [("ar", ma, 0, xr), ("ar", ma, 1, xl), ("y2", my, yo, xl)]
    order += [("bf", mb, 0, x2), ("bf", mb, 1, x2), ("y3", my, yo, x)]
    order += [("yx2", my, yh, x2), ("bn", mb, 1, xr), ("bn", mb, 0, xl)]
    order += [("br", mb, 0, xr), ("br", mb, 1, xl), ("yx", my, yh, xr)]
    order += [("yx", my, yh, xl), ("ao", ma, 0, x), ("ao", ma, 1, x)]
    order += [("bo", mb, 0, x), ("bo", mb, 1, x), ("yo", my, yh, x)]
    def load(src, dst, sem):
        pltpu.make_async_copy(src, dst, local_sem.at[sem]).start()

    def loaded(ref, sem):
        pltpu.make_async_copy(ref, ref, local_sem.at[sem]).wait()

    early, outs = {"af": ma, "an": ma, "y0": my}, {}
    for i, (tag, t, y, xx) in enumerate(order):
        if tag in early:
            n = len([k for k in outs if order[k][1] is t])
            outs[i] = (a_out if t is ma else y_out).at[n]
            load(t.share(t.slope.at[0], owner(y, xx, 1 - core)), outs[i], 0 if t is ma else 1)
    for tag, t, y, xx in order:
        load(t.share(t.slope.at[0], owner(y, xx, core)), t.s.at[y, xx], (ma, my, mb).index(t) + 2)
    for i, t in enumerate((ma, mb, my)):
        load(t.param, t.p, 5 + i)
    load(pn, pn_here, 8)
    load(sn, sn_here, 9)
    loaded(a_out, 0)
    loaded(y_out, 1)
    pl.semaphore_wait(barrier, 7)

    for i, (tag, t, y, xx) in enumerate(order):
        src = outs[i] if i in outs else t.share(t.slope.at[0], owner(y, xx, 1 - core))
        net.start(src, t.r.at[y, xx], partner, "swap" + "amby"[(ma, mb, my).index(t)], tag)
        if tag == "y2":
            net.start(sn, sn_other, partner, "sn", "sn")
            signal(hop_sem.at[0], up, down)
    for i, t in enumerate((ma, my, mb)):
        loaded(t.s, 2 + i)

    taken = [0]

    def take(tag):
        end = max(i for i, entry in enumerate(order) if entry[0] == tag) + 1
        for i in range(taken[0], end):
            name, t, y, xx = order[i]
            group = [j for j, entry in enumerate(order) if entry[0] == name]
            if i == group[0]:
                net.here(name, t.s.at[0, pl.ds(0, len(group))])
            add(t.s.at[y, xx], t.r.at[y, xx])
        taken[0] = max(taken[0], end)

    def x_send(t, h, xx, slot, target, stage):
        net.start(t.item(yh, h, xx), t.x_in.at[slot], target, t.name + "x", t.name + stage)

    def far(t):
        x_send(t, 0, x2, 0, right, "far")
        x_send(t, 1, x2, 1, left, "far")

    def near(t):
        x_send(t, 0, xl, 2, left, "near")
        x_send(t, 1, xr, 3, right, "near")

    def relay(t):
        net.here(t.name + "far", t.x_in.at[pl.ds(0, 2)])
        add(t.item(yh, 0, xr), t.x_in.at[0])
        x_send(t, 0, xr, 4, right, "near")
        add(t.item(yh, 1, xl), t.x_in.at[1])
        x_send(t, 1, xl, 5, left, "near")

    def settle(t):
        net.here(t.name + "near", t.x_in.at[pl.ds(2, 4)])
        for h in (0, 1):
            add(t.item(yh, h, x), t.x_in.at[2 + h], t.x_in.at[4 + h])

    def finish(t, extra=()):
        own = t.sums(yh, x)
        value = own[...]
        for e in extra:
            value = value + e[...]
        value = value * (replicas**-0.5)
        own[...] = value
        t.src[0:1, :] = t.squares(value)
        for k, peer in enumerate(others, 1):
            net.start(t.src, t.nm.at[k], peer, t.name + "norm", t.name + "norm")

    def update(t):
        total = t.src[...]
        net.here(t.name + "norm", t.nm.at[pl.ds(1, models - 1)])
        for k in range(1, models):
            total = total + t.nm[k]
        ratio = jnp.sqrt(total[1:2]) * lax.rsqrt(total[0:1] + EPS)
        if t.by_rows:
            ratio = jnp.broadcast_to(ratio, (ROWS, ROWS)).T[: t.rows]
            ratio = jnp.concatenate([ratio] * (t.p.shape[1] // ROWS), axis=1)
        new = t.p[...] - LEARN_RATE * (t.sums(yh, x)[...] * ratio)
        t.new[...] = new
        t.block(owner(yh, x, core))[...] = new.astype(jnp.bfloat16)

    def spread(t, y, xx, target, got):
        block = t.block(owner(y, xx, core))
        net.start(block, block, target, t.name + "half", t.name + got)

    def hand(t, y, xx):
        block = t.block(owner(y, xx, core))
        net.start(block, block, partner, t.name + "hand", t.name + "hand")

    def around(t, y, got):
        spread(t, y, x, right, got)
        spread(t, y, x, left, got)
        if t.direct:
            spread(t, y, x, beyond, got + "2")

    def wait(t, got, count):
        net.here(t.name + got, t.blocks(count))

    def rise(t):
        net.start(t.sums(yo, x), t.y, across, t.name + "y", t.name + "y")

    def risen(t):
        net.here(t.name + "y", t.y)
        finish(t, (t.y,))

    def y_send(xx, j):
        net.start(my.s.at[yo, xx], y_in.at[j], across, "y", "in%d" % j)

    def fold(xx, j):
        net.here("in%d" % j, y_in.at[j])
        add(my.s.at[yh, xx], y_in.at[j])

    def turn(xx, j):
        net.start(b4.sums(yo, xx), b4_in.at[j], across, "b4y", "b4in%d" % j)

    def turned(xx, j):
        net.here("b4in%d" % j, b4_in.at[j])
        add(b4.sums(yh, xx), b4_in.at[j])

    def publish(t):
        update(t)
        spread(t, yh, x, across, "up")
        hand(t, yh, x)

    def second(t):
        wait(t, "up", 1)
        around(t, yo, "oth")
        hand(t, yo, x)

    def pass_own(t):
        wait(t, "own", 2)
        if not t.direct:
            spread(t, yh, xl, right, "own2")
        hand(t, yh, xl)
        hand(t, yh, xr)

    def pass_oth(t):
        wait(t, "oth", 2)
        if not t.direct:
            spread(t, yo, xr, left, "oth2")
        hand(t, yo, xl)
        hand(t, yo, xr)

    def last(t, y, got):
        wait(t, got, 1)
        hand(t, y, x2)

    def publish_y(t):
        update(t)
        around(t, yh, "own")
        spread(t, yh, x, across, "up0")
        hand(t, yh, x)

    def climb(t):
        wait(t, "own", 2)
        spread(t, yh, xl, across, "up1")
        spread(t, yh, xr, across, "up1")
        hand(t, yh, xl)
        hand(t, yh, xr)

    def climb2(t):
        wait(t, "own2", 1)
        spread(t, yh, x2, across, "up2")
        hand(t, yh, x2)

    def tell(y, target, got):
        row = gain.at[core, y * XS + x]
        net.start(row, row, target, "tell", got)

    def told(got, count):
        net.here(got, gain.at[0, pl.ds(0, count)])

    take("af")
    far(a1)
    far(a2)
    take("y0")
    y_send(x2, 0)
    take("an")
    near(a1)
    near(a2)
    take("y1")
    y_send(xr, 1)
    take("ar")
    take("y2")
    y_send(xl, 2)
    for i, t in enumerate((ma, mb, my)):
        loaded(t.p, 5 + i)
    for t in (ta, b1, b2, y1, y2):
        t.src[1:2, :] = t.squares(t.p[...])
    take("bf")
    relay(a1)
    take("yx2")
    relay(a2)
    loaded(sn_here, 9)
    net.here("sn", sn_other)
    for y in (0, 1):
        for xx in range(XS):
            at = pl.ds(pl.multiple_of(owner(y, xx, core) * ROWS, ROWS), ROWS)
            tn.s[y, xx] = sn_here[0:1, at] + sn_other[0:1, at]
    far(tn)
    near(tn)
    far(b1)
    far(b3)
    pl.semaphore_wait(hop_sem.at[0], 2)
    signal(hop_sem.at[1], up, down)
    take("bn")
    near(b1)
    fold(x2, 0)
    pl.semaphore_wait(hop_sem.at[1], 2)
    signal(hop_sem.at[2], up, down)
    take("yo")
    pl.semaphore_wait(hop_sem.at[2], 2)
    signal(hop_sem.at[3], beside)
    turn(x2, 0)
    turn(xr, 1)
    turn(xl, 2)
    fold(xr, 1)
    net.gone("sn", sn_other)
    for name, t in (("swapa", ma), ("swapm", mb), ("swapb", my)):
        net.gone(name, t.s)
    settle(a1)
    rise(a1)
    settle(a2)
    rise(a2)
    y_send(x, 3)
    turn(x, 3)
    relay(tn)
    fold(xl, 2)
    relay(b1)
    near(b3)
    turned(x2, 0)
    far(b4)
    relay(b3)
    turned(xr, 1)
    turned(xl, 2)
    near(b4)
    far(y1)
    far(y2)
    near(y1)
    near(y2)
    pl.semaphore_wait(hop_sem.at[3], 1)
    for t in (a1, a2):
        net.gone(t.name + "x", t.x_in)
        net.here(t.name + "y", t.y)
        add(t.sums(yh, x), t.y)
    finish(ta)
    settle(b1)
    rise(b1)
    publish(ta)
    settle(b3)
    rise(b3)
    relay(b4)
    relay(y1)
    risen(b1)
    relay(y2)
    around(ta, yh, "own")
    settle(tn)
    net.start(tn.s.at[yo, x], tn.y, across, "ny", "ny")
    fold(x, 3)
    turned(x, 3)
    settle(b4)
    net.here("b3y", b3.y)
    add(b3.sums(yh, x), b3.y)
    finish(b2)
    settle(y1)
    finish(y1)
    settle(y2)
    finish(y2)
    second(ta)
    publish(b1)
    around(b1, yh, "own")
    loaded(pn_here, 8)
    net.here("ny", tn.y)
    add(tn.s.at[yh, x], tn.y)
    gain[core, yh * XS + x] = pn_here[...] - LEARN_RATE * (tn.s[yh, x] * (replicas**-0.5))
    nn[...] = gain[core, yh * XS + x]
    tell(yh, across, "nup")
    for target, got in ((right, "nown"), (left, "nown"), (beyond, "nown2")):
        tell(yh, target, got)
    pass_own(ta)
    for t in (a1, a2, b1, b3):
        net.gone(t.name + "y", t.y)
    net.gone("b4y", b4_in)
    net.gone("ny", tn.y)
    net.gone("y", y_in)
    net.gone("nx", tn.x_in)
    publish(b2)
    publish_y(y1)
    publish_y(y2)
    around(b2, yh, "own")
    pass_oth(ta)
    second(b1)
    pass_own(b1)
    told("nup", 1)
    for target, got in ((right, "noth"), (left, "noth"), (beyond, "noth2")):
        tell(yo, target, got)
    for t in (ta, b1, b2, y1, y2):
        net.gone(t.name + "norm", t.nm.at[pl.ds(1, models - 1)])
    for t in (b1, b3, b4, y1, y2):
        net.gone(t.name + "x", t.x_in)
    second(b2)
    climb(y1)
    climb2(y1)
    climb(y2)
    climb2(y2)
    pass_own(b2)
    pass_oth(b1)
    last(ta, yh, "own2")
    last(ta, yo, "oth2")
    told("nown", 2)
    told("nown2", 1)
    told("noth", 2)
    told("noth2", 1)
    net.start(gain.at[core], gain.at[core], partner, "nhand", "nhand")
    pass_oth(b2)
    for t in (y1, y2):
        wait(t, "up0", 1)
        hand(t, yo, x)
    net.here("nhand", gain.at[core])
    for y in (0, 1):
        for xx in range(XS):
            for c in (0, 1):
                at = owner(y, xx, c) * ROWS
                hn[at : at + ROWS] = gain[c, y * XS + xx, 0, :].astype(jnp.bfloat16)
    net.gone("nhand", gain.at[core])
    net.gone("tell", gain.at[0, pl.ds(0, 7)])
    net.gone("ahalf", ta.blocks(7))
    last(b1, yh, "own2")
    net.here("ahand", ta.blocks(8))
    net.gone("ahand", ta.blocks(8))

    def top(t):
        wait(t, "up1", 2)
        hand(t, yo, xl)
        hand(t, yo, xr)

    top(y1)
    last(b1, yo, "oth2")
    last(b2, yh, "own2")
    top(y2)
    last(y1, yo, "up2")
    last(b2, yo, "oth2")
    last(y2, yo, "up2")
    for t in (b1, y1, b2, y2):
        net.here(t.name + "hand", t.blocks(8))
        net.gone(t.name + "half", t.blocks(7))
        net.gone(t.name + "hand", t.blocks(8))


def store(*refs):
    copies = [
        pltpu.make_async_copy(refs[i], refs[8 + i], refs[16].at[i]) for i in range(8)
    ]
    for copy in copies:
        copy.start()
    for copy in copies:
        copy.wait()


def body(sg, su, sd, sn, pg, pu, pd, pn):
    arrays = (sg, su, sd, sn, pg, pu, pd, pn.reshape(1, ROWS))
    replicas, models = lax.axis_size("replica"), lax.axis_size("model")
    width, cols = sg.shape[1:]
    f32, bf16 = jnp.float32, jnp.bfloat16

    def matrix(share):
        sums = pltpu.VMEM((2, XS, *share), f32)
        return [sums, sums, pltpu.VMEM(share, f32)]

    def scratch(block, x_first):
        item = block if x_first else (block[0] // 2, block[1])
        arrived = [pltpu.VMEM((6, *item), f32)] + [pltpu.VMEM(block, f32)] * x_first
        return arrived + [pltpu.VMEM((2, ROWS), f32), pltpu.VMEM((models, 2, ROWS), f32)]

    vmem = pl.BlockSpec(memory_space=pltpu.VMEM)
    hbm = pl.BlockSpec(memory_space=pltpu.HBM)
    shape = jax.ShapeDtypeStruct
    out = pl.pallas_call(
        functools.partial(kernel, replicas, models),
        out_shape=(
            shape((width, cols), bf16),
            shape((width, cols), bf16),
            shape((cols, width), bf16),
            shape((width,), bf16),
            shape((ROWS, cols), f32),
            shape((ROWS, cols), f32),
            shape((cols, ROWS), f32),
            shape((1, ROWS), f32),
        ),
        in_specs=[hbm] * 8,
        out_specs=(vmem,) * 8,
        scratch_shapes=[
            *matrix((ROWS, cols)),
            *matrix((ROWS, cols)),
            *matrix((cols, ROWS)),
            *scratch((cols // 2, ROWS), True),
            *scratch((cols // 2, ROWS), True)[:2],
            *scratch((ROWS // 2, cols), True),
            *scratch((ROWS // 2 - TURNED, cols), True),
            pltpu.VMEM((6, TURNED // 2, cols), f32),
            pltpu.VMEM((XS, TURNED, cols), f32),
            *scratch((ROWS // 2, cols), False),
            *scratch((ROWS // 2, cols), False),
            pltpu.VMEM((XS, ROWS, cols), f32),
            pltpu.VMEM((2, XS, 1, ROWS), f32),
            pltpu.VMEM((6, 1, ROWS), f32),
            pltpu.VMEM((1, ROWS), f32),
            pltpu.VMEM((2, 2 * XS, 1, ROWS), f32),
            pltpu.VMEM((1, ROWS), f32),
            pltpu.VMEM((1, width), f32),
            pltpu.VMEM((1, width), f32),
            pltpu.VMEM((4, cols, ROWS), f32),
            pltpu.VMEM((1, ROWS, cols), f32),
            pltpu.SemaphoreType.DMA((10,)),
            pltpu.SemaphoreType.DMA((SENDS,)),
            pltpu.SemaphoreType.DMA((RECVS,)),
            pltpu.SemaphoreType.REGULAR((4,)),
        ],
        compiler_params=pltpu.CompilerParams(
            collective_id=0, has_side_effects=True, vmem_limit_bytes=32 << 20
        ),
    )(*(pltpu.with_memory_space_constraint(a, pltpu.HBM) for a in arrays))
    out = (*out[:3], out[3].reshape(width), *out[4:])
    out = pl.pallas_call(
        store,
        out_shape=tuple(shape(o.shape, o.dtype) for o in out),
        in_specs=[vmem] * 8,
        out_specs=(hbm,) * 8,
        scratch_shapes=[pltpu.SemaphoreType.DMA((8,))],
        compiler_params=pltpu.CompilerParams(vmem_limit_bytes=8 << 20),
    )(*(pltpu.with_memory_space_constraint(o, pltpu.VMEM) for o in out))
    return (*out[:7], out[7].reshape(ROWS))


def solution(mesh):
    return jax.shard_map(
        body,
        mesh=mesh,
        in_specs=(
            P("replica", None, "model"),
            P("replica", None, "model"),
            P("replica", "model", None),
            P("replica", None),
            P("replica", "model"),
            P("replica", "model"),
            P("model", "replica"),
            P("replica"),
        ),
        out_specs=(
            P(None, "model"),
            P(None, "model"),
            P("model", None),
            P(),
            P("replica", "model"),
            P("replica", "model"),
            P("model", "replica"),
            P("replica"),
        ),
        check_vma=False,
    )
```
